8 devices in a mesh: dp: 1 (over z), tp: 8 (over y, x, core).
Axes of the slice: x: 2, y: 2, z: 1, core: 2. Of those that a mesh axis runs over, the one named last changes fastest.
Arguments:
- hidden: bfloat16 [256, 4, 8192], P('dp')
- w_head: bfloat16 [8192, 32000], P(None, 'tp')
- q_draft: float32 [256, 3, 32000], P(('dp', 'tp'))
- x_draft: int32 [256, 3], P('dp')
Outputs:
- output 1: float32 [256, 3], P(('dp', 'tp'))
- output 2: float32 [256], P(('dp', 'tp'))
- output 3: float32 [256, 3, 32000], P(('dp', 'tp'))
- output 4: float32 [256, 32000], P(('dp', 'tp'))
All inputs are finite; a program needn't handle non-finite values.
Results may differ from the reference program's by a relative error of at most 0.001.
Values are sent between devices in bfloat16 or wider.
A program may use at most 1 GiB of HBM per device.

```python
import jax
import jax.numpy as jnp
from jax import lax

BATCH = 256
DRAFT = 3
HIDDEN = 8192
VOCAB = 32000
INV_TEMP = 1.25


def draw_tokens(token_key):
    tokens = jax.random.randint(token_key, (BATCH, DRAFT), 0, VOCAB, dtype=jnp.int32)
    return tokens.at[0, 0].set(VOCAB - 1).at[0, 1].set(0)


def setup_inputs(seed: int = 0, part: int = 0) -> dict:
    root_key = jax.random.key(seed)
    shared_key, part_root = jax.random.split(root_key)
    part_key = jax.random.fold_in(part_root, part)
    key_hidden, key_draft, key_token = jax.random.split(part_key, 3)
    raw_hidden = jax.random.normal(key_hidden, (BATCH, DRAFT + 1, HIDDEN), jnp.float32)
    hidden = raw_hidden * lax.rsqrt(jnp.mean(raw_hidden * raw_hidden, axis=-1, keepdims=True) + 1e-6)
    w_head = jax.random.normal(shared_key, (HIDDEN, VOCAB), jnp.float32) * HIDDEN ** -0.5
    draft_logits = 1.25 * jax.random.normal(key_draft, (BATCH, DRAFT, VOCAB), jnp.float32)
    q_draft = jax.nn.softmax(draft_logits, axis=-1)
    return {"hidden": hidden.astype(jnp.bfloat16), "w_head": w_head.astype(jnp.bfloat16), "q_draft": q_draft, "x_draft": draw_tokens(key_token)}


def reference(hidden, w_head, q_draft, x_draft):
    def verify_one(seq_args):
        hidden_seq, q_seq, x_seq = seq_args
        logits = jnp.dot(hidden_seq, w_head, preferred_element_type=jnp.float32) * INV_TEMP
        row_peak = jnp.max(logits, axis=-1, keepdims=True)
        exp_vals = jnp.exp(logits - row_peak)
        target_p = exp_vals / jnp.sum(exp_vals, axis=-1, keepdims=True)
        draft_p = target_p[:DRAFT]
        p_pick = jnp.take_along_axis(draft_p, x_seq[:, None], axis=1)[:, 0]
        q_pick = jnp.take_along_axis(q_seq, x_seq[:, None], axis=1)[:, 0]
        seq_accept = jnp.minimum(1.0, p_pick / q_pick)
        seq_expected = jnp.sum(jnp.cumprod(seq_accept))
        excess = jnp.maximum(draft_p - q_seq, 0.0)
        seq_resid = excess / jnp.sum(excess, axis=-1, keepdims=True)
        return seq_accept, seq_expected, seq_resid, target_p[DRAFT]

    accept, expected, residual, bonus = lax.map(verify_one, (hidden, q_draft, x_draft))
    return accept, expected, residual, bonus
```

```python
import functools

import jax
import jax.numpy as jnp
from jax import lax
from jax.experimental import pallas as pl
from jax.experimental.pallas import tpu as pltpu
from jax.sharding import PartitionSpec as P

INV_TEMP = 1.25
MESH = pl.DeviceIdType.MESH
LANE = 128
TILE = 256
HALVES = 2
SLOTS = 3
ORDER = (6, 2, 4, 7, 3, 5, 1)


def peer_of(me, k):
    d = me
    for bit in (1, 2, 4):
        if k & bit:
            d = d + bit * (1 - 2 * ((me // bit) % 2))
    return d


def logits_kernel(h_ref, w_ref, recv_ref, h_buf, w_buf, send_buf, h_sem, w_sem, own_sem, send_sem, recv_sem):
    me = lax.axis_index("tp")
    vocab = w_ref.shape[0]
    rows = h_buf.shape[1]
    seg = rows // 8
    n_tiles = pl.cdiv(vocab, TILE)
    last = vocab - (n_tiles - 1) * TILE
    lt = TILE // LANE

    def w_copy(t, size):
        slot = lax.rem(t, SLOTS)
        return pltpu.make_async_copy(w_ref.at[pl.ds(pl.multiple_of(t * TILE, TILE), size)], w_buf.at[slot, pl.ds(0, size)], w_sem.at[slot])

    def w_start(t):
        @pl.when(t < n_tiles - 1)
        def _():
            w_copy(t, TILE).start()

        @pl.when(t == n_tiles - 1)
        def _():
            w_copy(t, last).start()

    def w_wait(t):
        @pl.when(t < n_tiles - 1)
        def _():
            w_copy(t, TILE).wait()

        @pl.when(t == n_tiles - 1)
        def _():
            w_copy(t, last).wait()

    def h_start(half):
        for d in range(8):
            src = h_ref.at[pl.ds((d * HALVES + half) * seg, seg)]
            pltpu.make_async_copy(src, h_buf.at[half, pl.ds(d * seg, seg)], h_sem.at[half]).start()

    def h_wait(half):
        pltpu.make_async_copy(h_ref.at[pl.ds(0, rows)], h_buf.at[half], h_sem.at[half]).wait()

    h_start(0)
    w_copy(0, TILE).start()
    h_start(1)
    w_copy(1, TILE).start()

    barrier = pltpu.get_barrier_semaphore()
    for k in range(1, 8):
        pl.semaphore_signal(barrier, inc=1, device_id={"tp": peer_of(me, k)}, device_id_type=MESH)
    pl.semaphore_wait(barrier, 7)

    def step(i, carry):
        t = i // HALVES
        half = lax.rem(i, HALVES)
        slot = lax.rem(t, SLOTS)

        @pl.when(half == 0)
        def _():
            w_wait(t)

            @pl.when(t + 2 < n_tiles)
            def _():
                w_start(t + 2)

        @pl.when(i == 0)
        def _():
            h_wait(0)

        @pl.when(i == 1)
        def _():
            h_wait(1)

        z = lax.dot_general(h_buf[half], w_buf[slot], (((1,), (1,)), ((), ())), preferred_element_type=jnp.float32) * INV_TEMP
        for c in range(lt):
            send_buf[i, c] = z[:, c * LANE:(c + 1) * LANE]
        for k in ORDER:
            d = peer_of(me, k)
            pltpu.make_async_remote_copy(
                src_ref=send_buf.at[i, :, pl.ds(pl.multiple_of(d * seg, seg), seg)],
                dst_ref=recv_ref.at[me, pl.ds(t * lt, lt), half],
                send_sem=send_sem.at[k - 1],
                recv_sem=recv_sem.at[k - 1],
                device_id={"tp": d},
                device_id_type=MESH,
            ).start()
        pltpu.make_async_copy(
            send_buf.at[i, :, pl.ds(pl.multiple_of(me * seg, seg), seg)],
            recv_ref.at[me, pl.ds(t * lt, lt), half],
            own_sem.at[0],
        ).start()
        return carry

    lax.fori_loop(0, n_tiles * HALVES, step, 0)

    pltpu.make_async_copy(recv_ref.at[me], recv_ref.at[me], own_sem.at[0]).wait()
    for k in ORDER:
        d = peer_of(me, k)
        done = pltpu.make_async_remote_copy(
            src_ref=recv_ref.at[d],
            dst_ref=recv_ref.at[d],
            send_sem=send_sem.at[k - 1],
            recv_sem=recv_sem.at[k - 1],
            device_id={"tp": d},
            device_id_type=MESH,
        )
        done.wait_send()
        done.wait_recv()


def verify_kernel(x_ref, z_ref, q_ref, res_ref, bonus_ref, acc_ref, exp_ref):
    i = pl.program_id(0)
    n_src, n_lt = z_ref.shape[0], z_ref.shape[1]
    draft = q_ref.shape[0]
    vocab = q_ref.shape[2]
    shard = vocab // n_src
    seqs = q_ref.shape[1]
    n_out = acc_ref.shape[1]
    stride = draft + 1
    lane = lax.broadcasted_iota(jnp.int32, (seqs, LANE), 1)
    row = lax.broadcasted_iota(jnp.int32, (seqs, LANE), 0)
    tail = shard - (n_lt - 1) * LANE

    def tile(j, s, c):
        return z_ref[s, c, 0, pl.ds(j, seqs, stride=stride), :]

    wide = lax.broadcasted_iota(jnp.int32, (seqs, n_out), 1)
    deep = lax.broadcasted_iota(jnp.int32, (seqs, n_out), 0)
    accepts = []
    for j in range(stride):
        peak = None
        for s in range(n_src):
            for c in range(n_lt):
                z = tile(j, s, c)
                if c == n_lt - 1 and tail < LANE:
                    z = jnp.where(lane < tail, z, -jnp.inf)
                peak = z if peak is None else jnp.maximum(peak, z)
        peak = jnp.broadcast_to(jnp.max(peak, axis=1, keepdims=True), (seqs, LANE))
        out = (lambda g, v, j=j: res_ref.__setitem__((j, slice(None), slice(g * LANE, (g + 1) * LANE)), v)) if j < draft else (
            lambda g, v: bonus_ref.__setitem__((slice(None), slice(g * LANE, (g + 1) * LANE)), v))
        got = (lambda g, j=j: res_ref[j, :, g * LANE:(g + 1) * LANE]) if j < draft else (lambda g: bonus_ref[:, g * LANE:(g + 1) * LANE])
        total = jnp.zeros((seqs, LANE), jnp.float32)
        pend = None
        for s in range(n_src):
            off = s * shard % LANE
            base = s * shard // LANE
            for c in range(n_lt):
                e = jnp.exp(tile(j, s, c) - peak)
                if c == n_lt - 1 and tail < LANE:
                    e = jnp.where(lane < tail, e, 0.0)
                total = total + e
                r = pltpu.roll(e, off, 1) if off else e
                v = jnp.where(lane < off, pend, r) if off else r
                if c == n_lt - 1 and off + tail < LANE:
                    pend = v
                else:
                    out(base + c, v)
                    pend = r
        inv = jnp.broadcast_to(1.0 / jnp.sum(total, axis=1, keepdims=True), (seqs, LANE))
        n_g = vocab // LANE
        if j == draft:
            for g in range(n_g):
                out(g, got(g) * inv)
            continue
        excess = jnp.zeros((seqs, LANE), jnp.float32)
        for g in range(n_g):
            excess = excess + jnp.maximum(got(g) * inv - q_ref[j, :, g * LANE:(g + 1) * LANE], 0.0)
        p_pick = jnp.zeros((seqs, LANE), jnp.float32)
        q_pick = jnp.zeros((seqs, LANE), jnp.float32)
        for b in range(seqs):
            x = x_ref[(i * seqs + b) * draft + j]
            at = pl.multiple_of((x // LANE) * LANE, LANE)
            hit = (row == b) & (lane == x - at)
            p_pick = p_pick + jnp.where(hit, res_ref[j, :, pl.ds(at, LANE)], 0.0)
            q_pick = q_pick + jnp.where(hit, q_ref[j, :, pl.ds(at, LANE)], 0.0)
        p_col = jnp.sum(p_pick * inv, axis=1, keepdims=True)
        q_col = jnp.sum(q_pick, axis=1, keepdims=True)
        accepts.append(jnp.minimum(1.0, p_col / q_col))
        scale = jnp.broadcast_to(1.0 / jnp.sum(excess, axis=1, keepdims=True), (seqs, LANE))
        for g in range(n_g):
            out(g, jnp.maximum(got(g) * inv - q_ref[j, :, g * LANE:(g + 1) * LANE], 0.0) * scale)

    def to_lanes(col):
        return jnp.sum(jnp.where(wide == deep + i * seqs, jnp.broadcast_to(col, (seqs, n_out)), 0.0), axis=0, keepdims=True)

    @pl.when(i == 0)
    def _():
        acc_ref[...] = jnp.zeros_like(acc_ref)
        exp_ref[...] = jnp.zeros_like(exp_ref)

    run = None
    expected = None
    for j in range(draft):
        acc_ref[j:j + 1, :] += to_lanes(accepts[j])
        run = accepts[j] if j == 0 else run * accepts[j]
        expected = run if j == 0 else expected + run
    exp_ref[...] += to_lanes(expected)


def solution(mesh):
    n = mesh.shape["tp"]

    def local_step(hidden, w_shard, q_rows, x_group):
        seq_dev, draft, vocab = q_rows.shape
        batch, pos, depth = hidden.shape
        shard = w_shard.shape[1]
        n_tiles = pl.cdiv(shard, TILE)
        n_lt = n_tiles * TILE // LANE
        rows = batch * pos // HALVES
        seg = rows // n
        part = seq_dev // HALVES

        h = hidden.reshape(batch * pos, depth)
        recv = pl.pallas_call(
            logits_kernel,
            out_shape=jax.ShapeDtypeStruct((n, n_lt, HALVES, seg, LANE), jnp.float32),
            in_specs=[pl.BlockSpec(memory_space=pl.ANY)] * 2,
            out_specs=pl.BlockSpec(memory_space=pl.ANY),
            scratch_shapes=[
                pltpu.VMEM((HALVES, rows, depth), jnp.bfloat16),
                pltpu.VMEM((SLOTS, TILE, depth), jnp.bfloat16),
                pltpu.VMEM((n_tiles * HALVES, TILE // LANE, rows, LANE), jnp.float32),
                pltpu.SemaphoreType.DMA((HALVES,)),
                pltpu.SemaphoreType.DMA((SLOTS,)),
                pltpu.SemaphoreType.DMA((1,)),
                pltpu.SemaphoreType.DMA((7,)),
                pltpu.SemaphoreType.DMA((7,)),
            ],
            compiler_params=pltpu.CompilerParams(collective_id=0, has_side_effects=True, vmem_limit_bytes=60 * 1024 * 1024),
            cost_estimate=pl.CostEstimate(flops=2 * batch * pos * depth * shard, bytes_accessed=2 * shard * depth, transcendentals=0),
            name="logits_exchange",
        )(h, w_shard.T)

        x_own = lax.dynamic_slice_in_dim(x_group, lax.axis_index("tp") * seq_dev, seq_dev, axis=0).reshape(-1)
        seqs = 8
        grid = seq_dev // seqs
        per = part // seqs
        q_t = q_rows.transpose(1, 0, 2)
        res, bonus, acc, expd = pl.pallas_call(
            verify_kernel,
            grid_spec=pltpu.PrefetchScalarGridSpec(
                num_scalar_prefetch=1,
                grid=(grid,),
                in_specs=[
                    pl.BlockSpec((n, n_lt, 1, seqs * pos, LANE), lambda i, x: (0, 0, i // per, i % per, 0)),
                    pl.BlockSpec((draft, seqs, vocab), lambda i, x: (0, i, 0)),
                ],
                out_specs=[
                    pl.BlockSpec((draft, seqs, vocab), lambda i, x: (0, i, 0)),
                    pl.BlockSpec((seqs, vocab), lambda i, x: (i, 0)),
                    pl.BlockSpec((draft, seq_dev), lambda i, x: (0, 0)),
                    pl.BlockSpec((1, seq_dev), lambda i, x: (0, 0)),
                ],
            ),
            out_shape=[
                jax.ShapeDtypeStruct((draft, seq_dev, vocab), jnp.float32),
                jax.ShapeDtypeStruct((seq_dev, vocab), jnp.float32),
                jax.ShapeDtypeStruct((draft, seq_dev), jnp.float32),
                jax.ShapeDtypeStruct((1, seq_dev), jnp.float32),
            ],
            compiler_params=pltpu.CompilerParams(dimension_semantics=("arbitrary",), vmem_limit_bytes=60 * 1024 * 1024),
            name="verify_rows",
        )(x_own, recv, q_t)
        return acc.T, expd.reshape(seq_dev), res.transpose(1, 0, 2), bonus

    return jax.shard_map(local_step, mesh=mesh,
                         in_specs=(P("dp", None, None), P(None, "tp"), P(("dp", "tp"), None, None), P("dp", None)),
                         out_specs=(P(("dp", "tp"), None), P(("dp", "tp")), P(("dp", "tp"), None, None), P(("dp", "tp"), None)),
                         check_vma=False)
```

```python
import functools

import jax
import jax.numpy as jnp
from jax import lax
from jax.experimental import pallas as pl
from jax.experimental.pallas import tpu as pltpu
from jax.sharding import PartitionSpec as P

INV_TEMP = 1.25
MESH = pl.DeviceIdType.MESH
LANE = 128
TILE = 256
SEQS = 8
SLOTS = 3
ORDER = (6, 2, 4, 7, 3, 5, 1)


def peer_of(me, k):
    d = me
    for bit in (1, 2, 4):
        if k & bit:
            d = d + bit * (1 - 2 * ((me // bit) % 2))
    return d


def logits_kernel(h_ref, w_ref, recv_ref, edge_ref, stage, h_buf, w_buf, send_buf, edge_buf, h_sem, w_sem, own_sem, send_sem, recv_sem,
                  edge_send, edge_recv):
    me = lax.axis_index("tp")
    vocab, depth = w_ref.shape
    n_dev = recv_ref.shape[1]
    groups = recv_ref.shape[0]
    seqs = stage.shape[0] // n_dev
    pos = stage.shape[1]
    seg = seqs * pos
    per_dev = groups * seqs
    n_tiles = pl.cdiv(vocab, TILE)
    last = vocab - (n_tiles - 1) * TILE
    lt = TILE // LANE
    full = vocab // LANE
    tail = vocab - full * LANE
    n_steps = groups * n_tiles
    lane = lax.broadcasted_iota(jnp.int32, (seqs, LANE), 1)

    def w_copy(u, size):
        slot = lax.rem(u, SLOTS)
        t = lax.rem(u, n_tiles)
        return pltpu.make_async_copy(w_ref.at[pl.ds(pl.multiple_of(t * TILE, TILE), size)], w_buf.at[slot, pl.ds(0, size)], w_sem.at[slot])

    def on_tile(u, act):
        t = lax.rem(u, n_tiles)

        @pl.when(t < n_tiles - 1)
        def _():
            act(w_copy(u, TILE))

        @pl.when(t == n_tiles - 1)
        def _():
            act(w_copy(u, last))

    def h_copy(g, d):
        src = h_ref.at[pl.ds(d * per_dev + g * seqs, seqs)]
        return pltpu.make_async_copy(src, stage.at[pl.ds(d * seqs, seqs)], h_sem.at[d])

    def h_start(g):
        for d in range(n_dev):
            h_copy(g, d).start()

    def relayout(g):
        for d in range(n_dev):
            h_copy(g, d).wait()

            def cols(c, carry):
                at = pl.ds(pl.multiple_of(c * LANE, LANE), LANE)
                h_buf[pl.ds(d * seg, seg), at] = stage[pl.ds(d * seqs, seqs), :, at].reshape(seg, LANE)
                return carry

            lax.fori_loop(0, depth // LANE, cols, 0, unroll=8)

    h_start(0)
    w_copy(0, TILE).start()
    w_copy(1, TILE).start()

    barrier = pltpu.get_barrier_semaphore()
    for k in range(1, n_dev):
        pl.semaphore_signal(barrier, inc=1, device_id={"tp": peer_of(me, k)}, device_id_type=MESH)

    relayout(0)
    h_start(1)
    pl.semaphore_wait(barrier, n_dev - 1)

    def send(u, g, t, width):
        def rows(d):
            return pl.ds(pl.multiple_of(d * seg, seg), seg)

        dst = recv_ref.at[g, me, pl.ds(t * lt, width)]
        for k in ORDER:
            d = peer_of(me, k)
            pltpu.make_async_remote_copy(
                src_ref=send_buf.at[u, pl.ds(0, width), rows(d)],
                dst_ref=dst,
                send_sem=send_sem.at[k - 1],
                recv_sem=recv_sem.at[k - 1],
                device_id={"tp": d},
                device_id_type=MESH,
            ).start()
        pltpu.make_async_copy(send_buf.at[u, pl.ds(0, width), rows(me)], dst, own_sem.at[0]).start()

    def send_edge(u, g):
        for d in range(n_dev):
            packed = jnp.zeros((seqs, LANE), jnp.float32)
            for j in range(pos):
                v = send_buf[u, 1, pl.ds(d * seg + j, seqs, stride=pos), :]
                v = pltpu.roll(v, j * tail, 1) if j else v
                packed = jnp.where((lane >= j * tail) & (lane < (j + 1) * tail), v, packed)
            edge_buf[g, d] = packed
        for k in ORDER:
            d = peer_of(me, k)
            pltpu.make_async_remote_copy(
                src_ref=edge_buf.at[g, d],
                dst_ref=edge_ref.at[g, me],
                send_sem=edge_send.at[k - 1],
                recv_sem=edge_recv.at[k - 1],
                device_id={"tp": d},
                device_id_type=MESH,
            ).start()
        pltpu.make_async_copy(edge_buf.at[g, me], edge_ref.at[g, me], own_sem.at[1]).start()

    def step(u, carry):
        g = u // n_tiles
        t = lax.rem(u, n_tiles)
        slot = lax.rem(u, SLOTS)

        @pl.when((t == 0) & (g > 0))
        def _():
            relayout(g)

            @pl.when(g + 1 < groups)
            def _():
                h_start(g + 1)

        on_tile(u, lambda c: c.wait())

        @pl.when(u + 2 < n_steps)
        def _():
            on_tile(u + 2, lambda c: c.start())

        z = lax.dot_general(h_buf[...], w_buf[slot], (((1,), (1,)), ((), ())), preferred_element_type=jnp.float32) * INV_TEMP
        for c in range(lt):
            send_buf[u, c] = z[:, c * LANE:(c + 1) * LANE]

        @pl.when(t < n_tiles - 1)
        def _():
            send(u, g, t, lt)

        @pl.when(t == n_tiles - 1)
        def _():
            send(u, g, t, full - (n_tiles - 1) * lt)
            send_edge(u, g)

        return carry

    lax.fori_loop(0, n_steps, step, 0)

    pltpu.make_async_copy(recv_ref.at[:, me], recv_ref.at[:, me], own_sem.at[0]).wait()
    pltpu.make_async_copy(edge_ref.at[:, me], edge_ref.at[:, me], own_sem.at[1]).wait()
    for k in ORDER:
        d = peer_of(me, k)
        for ref, ss, rs in ((recv_ref, send_sem, recv_sem), (edge_ref, edge_send, edge_recv)):
            done = pltpu.make_async_remote_copy(
                src_ref=ref.at[:, d],
                dst_ref=ref.at[:, d],
                send_sem=ss.at[k - 1],
                recv_sem=rs.at[k - 1],
                device_id={"tp": d},
                device_id_type=MESH,
            )
            done.wait_send()
            done.wait_recv()


def verify_kernel(x_ref, z_ref, edge_ref, q_ref, res_ref, bonus_ref, acc_ref, exp_ref):
    i = pl.program_id(0)
    n_src, full = z_ref.shape[1], z_ref.shape[2]
    n_lt = full + 1
    draft = q_ref.shape[0]
    vocab = q_ref.shape[2]
    shard = vocab // n_src
    seqs = q_ref.shape[1]
    n_out = acc_ref.shape[1]
    stride = draft + 1
    lane = lax.broadcasted_iota(jnp.int32, (seqs, LANE), 1)
    row = lax.broadcasted_iota(jnp.int32, (seqs, LANE), 0)
    tail = shard - full * LANE

    def tile(j, s, c):
        if c < full:
            return z_ref[0, s, c, pl.ds(j, seqs, stride=stride), :]
        v = edge_ref[0, s]
        return pltpu.roll(v, LANE - j * tail, 1) if j else v

    wide = lax.broadcasted_iota(jnp.int32, (seqs, n_out), 1)
    deep = lax.broadcasted_iota(jnp.int32, (seqs, n_out), 0)
    accepts = []
    for j in range(stride):
        peak = None
        for s in range(n_src):
            for c in range(n_lt):
                z = tile(j, s, c)
                if c == n_lt - 1 and tail < LANE:
                    z = jnp.where(lane < tail, z, -jnp.inf)
                peak = z if peak is None else jnp.maximum(peak, z)
        peak = jnp.broadcast_to(jnp.max(peak, axis=1, keepdims=True), (seqs, LANE))
        out = (lambda g, v, j=j: res_ref.__setitem__((j, slice(None), slice(g * LANE, (g + 1) * LANE)), v)) if j < draft else (
            lambda g, v: bonus_ref.__setitem__((slice(None), slice(g * LANE, (g + 1) * LANE)), v))
        got = (lambda g, j=j: res_ref[j, :, g * LANE:(g + 1) * LANE]) if j < draft else (lambda g: bonus_ref[:, g * LANE:(g + 1) * LANE])
        total = jnp.zeros((seqs, LANE), jnp.float32)
        pend = None
        for s in range(n_src):
            off = s * shard % LANE
            base = s * shard // LANE
            for c in range(n_lt):
                e = jnp.exp(tile(j, s, c) - peak)
                if c == n_lt - 1 and tail < LANE:
                    e = jnp.where(lane < tail, e, 0.0)
                total = total + e
                r = pltpu.roll(e, off, 1) if off else e
                v = jnp.where(lane < off, pend, r) if off else r
                if c == n_lt - 1 and off + tail < LANE:
                    pend = v
                else:
                    out(base + c, v)
                    pend = r
        inv = jnp.broadcast_to(1.0 / jnp.sum(total, axis=1, keepdims=True), (seqs, LANE))
        n_g = vocab // LANE
        if j == draft:
            for g in range(n_g):
                out(g, got(g) * inv)
            continue
        excess = jnp.zeros((seqs, LANE), jnp.float32)
        for g in range(n_g):
            excess = excess + jnp.maximum(got(g) * inv - q_ref[j, :, g * LANE:(g + 1) * LANE], 0.0)
        p_pick = jnp.zeros((seqs, LANE), jnp.float32)
        q_pick = jnp.zeros((seqs, LANE), jnp.float32)
        for b in range(seqs):
            x = x_ref[(i * seqs + b) * draft + j]
            at = pl.multiple_of((x // LANE) * LANE, LANE)
            hit = (row == b) & (lane == x - at)
            p_pick = p_pick + jnp.where(hit, res_ref[j, :, pl.ds(at, LANE)], 0.0)
            q_pick = q_pick + jnp.where(hit, q_ref[j, :, pl.ds(at, LANE)], 0.0)
        p_col = jnp.sum(p_pick * inv, axis=1, keepdims=True)
        q_col = jnp.sum(q_pick, axis=1, keepdims=True)
        accepts.append(jnp.minimum(1.0, p_col / q_col))
        scale = jnp.broadcast_to(1.0 / jnp.sum(excess, axis=1, keepdims=True), (seqs, LANE))
        for g in range(n_g):
            out(g, jnp.maximum(got(g) * inv - q_ref[j, :, g * LANE:(g + 1) * LANE], 0.0) * scale)

    def to_lanes(col):
        return jnp.sum(jnp.where(wide == deep + i * seqs, jnp.broadcast_to(col, (seqs, n_out)), 0.0), axis=0, keepdims=True)

    @pl.when(i == 0)
    def _():
        acc_ref[...] = jnp.zeros_like(acc_ref)
        exp_ref[...] = jnp.zeros_like(exp_ref)

    run = None
    expected = None
    for j in range(draft):
        acc_ref[j:j + 1, :] += to_lanes(accepts[j])
        run = accepts[j] if j == 0 else run * accepts[j]
        expected = run if j == 0 else expected + run
    exp_ref[...] += to_lanes(expected)


def solution(mesh):
    n = mesh.shape["tp"]

    def local_step(hidden, w_shard, q_rows, x_group):
        seq_dev, draft, vocab = q_rows.shape
        batch, pos, depth = hidden.shape
        shard = w_shard.shape[1]
        n_tiles = pl.cdiv(shard, TILE)
        groups = seq_dev // SEQS
        rows = n * SEQS * pos
        full = shard // LANE
        recv, edge = pl.pallas_call(
            logits_kernel,
            out_shape=[
                jax.ShapeDtypeStruct((groups, n, full, SEQS * pos, LANE), jnp.float32),
                jax.ShapeDtypeStruct((groups, n, SEQS, LANE), jnp.float32),
            ],
            in_specs=[pl.BlockSpec(memory_space=pl.ANY)] * 2,
            out_specs=[pl.BlockSpec(memory_space=pl.ANY)] * 2,
            scratch_shapes=[
                pltpu.VMEM((n * SEQS, pos, depth), jnp.bfloat16),
                pltpu.VMEM((rows, depth), jnp.bfloat16),
                pltpu.VMEM((SLOTS, TILE, depth), jnp.bfloat16),
                pltpu.VMEM((groups * n_tiles, TILE // LANE, rows, LANE), jnp.float32),
                pltpu.VMEM((groups, n, SEQS, LANE), jnp.float32),
                pltpu.SemaphoreType.DMA((n,)),
                pltpu.SemaphoreType.DMA((SLOTS,)),
                pltpu.SemaphoreType.DMA((2,)),
                pltpu.SemaphoreType.DMA((n - 1,)),
                pltpu.SemaphoreType.DMA((n - 1,)),
                pltpu.SemaphoreType.DMA((n - 1,)),
                pltpu.SemaphoreType.DMA((n - 1,)),
            ],
            compiler_params=pltpu.CompilerParams(collective_id=0, has_side_effects=True, vmem_limit_bytes=60 * 1024 * 1024),
            cost_estimate=pl.CostEstimate(flops=2 * batch * pos * depth * shard, bytes_accessed=2 * shard * depth, transcendentals=0),
            name="logits_exchange",
        )(hidden, w_shard.T)

        x_own = lax.dynamic_slice_in_dim(x_group, lax.axis_index("tp") * seq_dev, seq_dev, axis=0).reshape(-1)
        seqs = SEQS
        q_t = q_rows.transpose(1, 0, 2)
        res, bonus, acc, expd = pl.pallas_call(
            verify_kernel,
            grid_spec=pltpu.PrefetchScalarGridSpec(
                num_scalar_prefetch=1,
                grid=(groups,),
                in_specs=[
                    pl.BlockSpec((1, n, full, seqs * pos, LANE), lambda i, x: (i, 0, 0, 0, 0)),
                    pl.BlockSpec((1, n, seqs, LANE), lambda i, x: (i, 0, 0, 0)),
                    pl.BlockSpec((draft, seqs, vocab), lambda i, x: (0, i, 0)),
                ],
                out_specs=[
                    pl.BlockSpec((draft, seqs, vocab), lambda i, x: (0, i, 0)),
                    pl.BlockSpec((seqs, vocab), lambda i, x: (i, 0)),
                    pl.BlockSpec((draft, seq_dev), lambda i, x: (0, 0)),
                    pl.BlockSpec((1, seq_dev), lambda i, x: (0, 0)),
                ],
            ),
            out_shape=[
                jax.ShapeDtypeStruct((draft, seq_dev, vocab), jnp.float32),
                jax.ShapeDtypeStruct((seq_dev, vocab), jnp.float32),
                jax.ShapeDtypeStruct((draft, seq_dev), jnp.float32),
                jax.ShapeDtypeStruct((1, seq_dev), jnp.float32),
            ],
            compiler_params=pltpu.CompilerParams(dimension_semantics=("arbitrary",), vmem_limit_bytes=60 * 1024 * 1024),
            name="verify_rows",
        )(x_own, recv, edge, q_t)
        return acc.T, expd.reshape(seq_dev), res.transpose(1, 0, 2), bonus

    return jax.shard_map(local_step, mesh=mesh,
                         in_specs=(P("dp", None, None), P(None, "tp"), P(("dp", "tp"), None, None), P("dp", None)),
                         out_specs=(P(("dp", "tp"), None), P(("dp", "tp")), P(("dp", "tp"), None, None), P(("dp", "tp"), None)),
                         check_vma=False)
```

```python
import jax
import jax.numpy as jnp
from jax import lax
from jax.experimental import pallas as pl
from jax.experimental.pallas import tpu as pltpu
from jax.sharding import PartitionSpec as P

INV_TEMP = 1.25
MESH = pl.DeviceIdType.MESH
LANE = 128
TILE = 256
SEQS = 8
SLOTS = 3
ORDER = (6, 2, 4, 7, 3, 5, 1)
CHAINS = 4
UNROLL = 25
MIB = 1024 * 1024
VMEM_A = 32
VMEM_B = 32


def peer_of(me, k):
    d = me
    for bit in (1, 2, 4):
        if k & bit:
            d = d + bit * (1 - 2 * ((me // bit) % 2))
    return d


def lanes(g):
    return pl.ds(pl.multiple_of(g * LANE, LANE), LANE)


def chained(op, n, unroll, term, parts):
    def body(c, parts):
        return (*parts[1:], op(parts[0], term(c)))

    return lax.fori_loop(0, n, body, parts, unroll=unroll)


def across(op, reduce, parts, shape):
    v = parts[0]
    for p in parts[1:]:
        v = op(v, p)
    return jnp.broadcast_to(reduce(v, axis=1, keepdims=True), shape)


def softmax_rows(tile, edge, put, n_src, full, tail, seqs):
    shard = full * LANE + tail
    shape = (seqs, LANE)
    lane = lax.broadcasted_iota(jnp.int32, shape, 1)
    parts = (tile(0, 0),) * CHAINS
    for s in range(n_src):
        parts = chained(jnp.maximum, full, full, lambda c: tile(s, c), parts)
        parts = (*parts[1:], jnp.maximum(parts[0], jnp.where(lane < tail, edge(s), -jnp.inf)))
    peak = across(jnp.maximum, jnp.max, parts, shape)
    pend = tile(0, 0) * 0.0
    parts = (pend,) * CHAINS
    for s in range(n_src):
        off = s * shard % LANE
        base = s * shard // LANE

        def place(i, e, pend):
            r = pltpu.roll(e, off, 1) if off else e
            v = jnp.where(lane < off, pend, r) if off else r
            return r, v

        def body(c, carry):
            pend, *parts = carry
            e = jnp.exp(tile(s, c) - peak)
            r, v = place(base + c, e, pend)
            put(base + c, v)
            return (r, *parts[1:], parts[0] + e)

        pend, *parts = lax.fori_loop(0, full, body, (pend, *parts), unroll=full)
        e = jnp.where(lane < tail, jnp.exp(edge(s) - peak), 0.0)
        parts = [*parts[1:], parts[0] + e]
        _, pend = place(base + full, e, pend)
        if off + tail == LANE:
            put(base + full, pend)
    return 1.0 / across(jnp.add, jnp.sum, parts, shape)


def finish_bonus(get, put, inv, n_g):
    def body(i, carry):
        put(i, get(i) * inv)
        return carry

    lax.fori_loop(0, n_g, body, 0, unroll=UNROLL)


def excess_rows(get, q_tile, inv, n_g):
    shape = inv.shape
    parts = chained(jnp.add, n_g, UNROLL, lambda i: jnp.maximum(get(i) * inv - q_tile(i), 0.0), (get(0) * 0.0,) * CHAINS)
    return 1.0 / across(jnp.add, jnp.sum, parts, shape)


def excess_rows_with_picks(get, q_tile, token, inv, n_g):
    shape = inv.shape
    lane = lax.broadcasted_iota(jnp.int32, shape, 1)
    row = lax.broadcasted_iota(jnp.int32, shape, 0)
    x = jnp.zeros(shape, jnp.int32)
    for b in range(shape[0]):
        x = jnp.where(row == b, token(b), x)
    x = x - lane

    def body(i, carry):
        p_pick, q_pick, *parts = carry
        p, q = get(i) * inv, q_tile(i)
        hit = x == i * LANE
        return (jnp.where(hit, p, p_pick), jnp.where(hit, q, q_pick), *parts[1:], parts[0] + jnp.maximum(p - q, 0.0))

    zero = get(0) * 0.0
    p_pick, q_pick, *parts = lax.fori_loop(0, n_g, body, (zero,) * (CHAINS + 2), unroll=UNROLL)
    return 1.0 / across(jnp.add, jnp.sum, parts, shape), accept_column(p_pick, q_pick)


def accept_column(p_pick, q_pick):
    return jnp.minimum(1.0, jnp.sum(p_pick, axis=1, keepdims=True) / jnp.sum(q_pick, axis=1, keepdims=True))


def picks_at(get_at, q_at, token, inv):
    shape = inv.shape
    lane = lax.broadcasted_iota(jnp.int32, shape, 1)
    row = lax.broadcasted_iota(jnp.int32, shape, 0)
    p_pick = jnp.zeros(shape, jnp.float32)
    q_pick = jnp.zeros(shape, jnp.float32)
    for b in range(shape[0]):
        x = token(b)
        at = pl.multiple_of((x // LANE) * LANE, LANE)
        hit = (row == b) & (lane == x - at)
        p_pick = jnp.where(hit, get_at(at) * inv, p_pick)
        q_pick = jnp.where(hit, q_at(at), q_pick)
    return accept_column(p_pick, q_pick)


def residual_rows(get, put, q_tile, inv, scale, n_g):
    def body(i, carry):
        put(i, jnp.maximum(get(i) * inv - q_tile(i), 0.0) * scale)
        return carry

    lax.fori_loop(0, n_g, body, 0, unroll=UNROLL)


def to_lanes(col, first, n_out):
    seqs = col.shape[0]
    wide = lax.broadcasted_iota(jnp.int32, (seqs, n_out), 1)
    deep = lax.broadcasted_iota(jnp.int32, (seqs, n_out), 0)
    return jnp.sum(jnp.where(wide == deep + first, jnp.broadcast_to(col, (seqs, n_out)), 0.0), axis=0, keepdims=True)


def prefixes(accepts):
    run, expected = accepts[0], accepts[0]
    for a in accepts[1:]:
        run = run * a
        expected = expected + run
    return expected


def exchange_kernel(x_ref, h_ref, w_ref, q_ref, recv_ref, edge_ref, done_ref, acc_ref, stage, h_buf, w_buf, z_buf, send_buf, edge_buf, q_buf,
                    h_sem, w_sem, q_sem, send_sem, recv_sem, edge_send, edge_recv):
    me = lax.axis_index("tp")
    vocab, depth = w_ref.shape
    groups, n_dev = recv_ref.shape[:2]
    seqs = stage.shape[0] // n_dev
    pos = stage.shape[1]
    draft = pos - 1
    seg = seqs * pos
    per_dev = groups * seqs
    n_tiles = pl.cdiv(vocab, TILE)
    last = vocab - (n_tiles - 1) * TILE
    lt = TILE // LANE
    full = vocab // LANE
    tail = vocab - full * LANE
    n_steps = groups * n_tiles
    lane = lax.broadcasted_iota(jnp.int32, (seqs, LANE), 1)

    def w_copy(u, size):
        slot = lax.rem(u, SLOTS)
        t = lax.rem(u, n_tiles)
        return pltpu.make_async_copy(w_ref.at[pl.ds(pl.multiple_of(t * TILE, TILE), size)], w_buf.at[slot, pl.ds(0, size)], w_sem.at[slot])

    def on_tile(u, act):
        t = lax.rem(u, n_tiles)

        @pl.when(t < n_tiles - 1)
        def _():
            act(w_copy(u, TILE))

        @pl.when(t == n_tiles - 1)
        def _():
            act(w_copy(u, last))

    def h_copy(g, d):
        src = h_ref.at[pl.ds(d * per_dev + g * seqs, seqs)]
        return pltpu.make_async_copy(src, stage.at[pl.ds(d * seqs, seqs)], h_sem.at[d])

    def h_start(g):
        for d in range(n_dev):
            h_copy(g, d).start()

    def relayout(g):
        for d in range(n_dev):
            h_copy(g, d).wait()

            def cols(c, carry):
                at = pl.ds(pl.multiple_of(c * LANE, LANE), LANE)
                h_buf[pl.ds(d * seg, seg), at] = stage[pl.ds(d * seqs, seqs), :, at].reshape(seg, LANE)
                return carry

            lax.fori_loop(0, depth // LANE, cols, 0, unroll=8)

    def q_copy(g, j):
        return pltpu.make_async_copy(q_ref.at[j, pl.ds(pl.multiple_of(g * seqs, seqs), seqs)], q_buf.at[j], q_sem.at[j])

    h_start(0)
    w_copy(0, TILE).start()
    w_copy(1, TILE).start()

    barrier = pltpu.get_barrier_semaphore()
    for k in range(1, n_dev):
        pl.semaphore_signal(barrier, inc=1, device_id={"tp": peer_of(me, k)}, device_id_type=MESH)

    acc_ref[...] = jnp.zeros_like(acc_ref)
    relayout(0)
    h_start(1)
    pl.semaphore_wait(barrier, n_dev - 1)

    def send(g, t, width):
        for c in range(width):
            recv_ref[g, me, t * lt + c] = send_buf[t, c, pl.ds(pl.multiple_of(me * seg, seg), seg), :]
        for k in ORDER:
            d = peer_of(me, k)
            pltpu.make_async_remote_copy(
                src_ref=send_buf.at[t, pl.ds(0, width), pl.ds(pl.multiple_of(d * seg, seg), seg)],
                dst_ref=recv_ref.at[g, me, pl.ds(t * lt, width)],
                send_sem=send_sem.at[t],
                recv_sem=recv_sem.at[g, k - 1],
                device_id={"tp": d},
                device_id_type=MESH,
            ).start()

    def wait_sent(t, width):
        ref = send_buf.at[t, pl.ds(0, width), pl.ds(0, (n_dev - 1) * seg)]
        pltpu.make_async_remote_copy(
            src_ref=ref, dst_ref=ref, send_sem=send_sem.at[t], recv_sem=recv_sem.at[0, 0],
            device_id={"tp": peer_of(me, 1)}, device_id_type=MESH,
        ).wait_send()

    def send_edge(g):
        for d in range(n_dev):
            packed = z_buf[1, pl.ds(d * seg, seqs, stride=pos), :]
            for j in range(1, pos):
                v = pltpu.roll(z_buf[1, pl.ds(d * seg + j, seqs, stride=pos), :], j * tail, 1)
                packed = jnp.where(lane < j * tail, packed, v)
            edge_buf[g, d] = packed
        edge_ref[g, me] = edge_buf[g, me]
        for k in ORDER:
            d = peer_of(me, k)
            pltpu.make_async_remote_copy(
                src_ref=edge_buf.at[g, d],
                dst_ref=edge_ref.at[g, me],
                send_sem=edge_send.at[k - 1],
                recv_sem=edge_recv.at[g, k - 1],
                device_id={"tp": d},
                device_id_type=MESH,
            ).start()

    rest = full - (n_tiles - 1) * lt

    def step(u, carry):
        g = u // n_tiles
        t = lax.rem(u, n_tiles)
        slot = lax.rem(u, SLOTS)

        @pl.when((t == 0) & (g > 0))
        def _():
            relayout(g)

            @pl.when(g + 1 < groups)
            def _():
                h_start(g + 1)

        on_tile(u, lambda c: c.wait())

        @pl.when(u + 2 < n_steps)
        def _():
            on_tile(u + 2, lambda c: c.start())

        z = lax.dot_general(h_buf[...], w_buf[slot], (((1,), (1,)), ((), ())), preferred_element_type=jnp.float32) * INV_TEMP
        for c in range(lt):
            z_buf[c] = z[:, c * LANE:(c + 1) * LANE]

        @pl.when((g > 0) & (t < n_tiles - 1))
        def _():
            wait_sent(t, lt)

        @pl.when((g > 0) & (t == n_tiles - 1))
        def _():
            wait_sent(t, rest)

        for c in range(lt):
            for d in range(n_dev):
                for j in range(pos):
                    send_buf[t, c, pl.ds(d * seg + j * seqs, seqs), :] = z_buf[c, pl.ds(d * seg + j, seqs, stride=pos), :]

        @pl.when(t < n_tiles - 1)
        def _():
            send(g, t, lt)

        @pl.when(t == n_tiles - 1)
        def _():
            send(g, t, rest)
            send_edge(g)

        return carry

    lax.fori_loop(0, n_steps, step, 0)

    def wait_group(g):
        for k in ORDER:
            d = peer_of(me, k)
            for ref, ss, rs in ((recv_ref, edge_send, recv_sem), (edge_ref, edge_send, edge_recv)):
                pltpu.make_async_remote_copy(
                    src_ref=ref.at[g, d], dst_ref=ref.at[g, d], send_sem=ss.at[k - 1], recv_sem=rs.at[g, k - 1],
                    device_id={"tp": d}, device_id_type=MESH,
                ).wait_recv()

    for j in range(draft):
        q_copy(0, j).start()

    def finish(g, carry):
        wait_group(g)
        accepts = []
        for j in range(pos):
            def tile(s, c):
                return recv_ref[g, s, c, pl.ds(j * seqs, seqs), :]

            def edge(s):
                v = edge_ref[g, s]
                return pltpu.roll(v, LANE - j * tail, 1) if j else v

            def put(i, v):
                done_ref[g, j, :, lanes(i)] = v

            def get(i):
                return done_ref[g, j, :, lanes(i)]

            n_g = done_ref.shape[3] // LANE
            inv = softmax_rows(tile, edge, put, n_dev, full, tail, seqs)
            if j == draft:
                finish_bonus(get, put, inv, n_g)
                continue
            q_copy(g, j).wait()
            def q_tile(i):
                return q_buf[j, :, lanes(i)]

            scale, accept = excess_rows_with_picks(get, q_tile, lambda b: x_ref[j, me * per_dev + g * seqs + b], inv, n_g)
            accepts.append(accept)
            residual_rows(get, put, q_tile, inv, scale, n_g)

            @pl.when(g + 2 < groups)
            def _():
                q_copy(g + 1, j).start()

        for j in range(draft):
            acc_ref[j:j + 1, :] += to_lanes(accepts[j], g * seqs, per_dev)
        acc_ref[draft:pos, :] += to_lanes(prefixes(accepts), g * seqs, per_dev)
        return carry

    lax.fori_loop(0, groups - 1, finish, 0)
    wait_group(groups - 1)

    for t in range(n_tiles):
        wait_sent(t, lt if t < n_tiles - 1 else rest)
    for k in ORDER:
        d = peer_of(me, k)
        ref = edge_ref.at[:, d]
        pltpu.make_async_remote_copy(
            src_ref=ref, dst_ref=ref, send_sem=edge_send.at[k - 1], recv_sem=edge_recv.at[0, k - 1],
            device_id={"tp": d}, device_id_type=MESH,
        ).wait_send()


def output_kernel(x_ref, recv_ref, edge_ref, done_ref, part_ref, q_ref, res_ref, bonus_ref, acc_ref, exp_ref, row_buf, q_buf, q_sem, out_sem):
    me = lax.axis_index("tp")
    groups, n_dev, full = recv_ref.shape[:3]
    seqs = edge_ref.shape[2]
    pos = done_ref.shape[1]
    draft = pos - 1
    vocab = done_ref.shape[3]
    n_g = vocab // LANE
    tail = vocab // n_dev - full * LANE
    per_dev = groups * seqs
    g_last = groups - 1

    def q_copy(j):
        return pltpu.make_async_copy(q_ref.at[j, pl.ds(g_last * seqs, seqs)], q_buf.at[j], q_sem.at[j])

    def out(g, j, src):
        dst = bonus_ref if j == draft else res_ref.at[j]
        return pltpu.make_async_copy(src, dst.at[pl.ds(g * seqs, seqs)], out_sem.at[g, j])

    for j in range(draft):
        q_copy(j).start()
    for g in range(g_last):
        for j in range(pos):
            out(g, j, done_ref.at[g, j]).start()

    accepts = []
    for j in (draft, *range(draft)):
        def tile(s, c):
            return recv_ref[g_last, s, c, pl.ds(j * seqs, seqs), :]

        def edge(s):
            v = edge_ref[g_last, s]
            return pltpu.roll(v, LANE - j * tail, 1) if j else v

        def put(i, v):
            row_buf[j, :, lanes(i)] = v

        def get(i):
            return row_buf[j, :, lanes(i)]

        inv = softmax_rows(tile, edge, put, n_dev, full, tail, seqs)
        if j == draft:
            finish_bonus(get, put, inv, n_g)
        else:
            q_copy(j).wait()
            def q_tile(i):
                return q_buf[j, :, lanes(i)]

            accepts.append(picks_at(
                lambda at: row_buf[j, :, pl.ds(at, LANE)], lambda at: q_buf[j, :, pl.ds(at, LANE)],
                lambda b: x_ref[j, me * per_dev + g_last * seqs + b], inv))
            residual_rows(get, put, q_tile, inv, excess_rows(get, q_tile, inv, n_g), n_g)
        out(g_last, j, row_buf.at[j]).start()

    for j in range(draft):
        acc_ref[j:j + 1, :] = part_ref[j:j + 1, :] + to_lanes(accepts[j], g_last * seqs, per_dev)
    exp_ref[...] = part_ref[draft:pos, :] + to_lanes(prefixes(accepts), g_last * seqs, per_dev)
    for g in range(groups):
        for j in range(pos):
            out(g, j, row_buf.at[j]).wait()


def solution(mesh):
    n = mesh.shape["tp"]

    def local_step(hidden, w_shard, q_rows, x_group):
        seq_dev, draft, vocab = q_rows.shape
        batch, pos, depth = hidden.shape
        shard = w_shard.shape[1]
        n_tiles = pl.cdiv(shard, TILE)
        groups = seq_dev // SEQS
        rows = n * SEQS * pos
        full = shard // LANE
        dma = pltpu.SemaphoreType.DMA
        in_hbm = pl.BlockSpec(memory_space=pltpu.HBM)
        in_vmem = pl.BlockSpec(memory_space=pltpu.VMEM)
        in_smem = pl.BlockSpec(memory_space=pltpu.SMEM)
        x_t = x_group.T
        q_hbm = pltpu.with_memory_space_constraint(q_rows.transpose(1, 0, 2), pltpu.HBM)

        recv, edge, done, part = pl.pallas_call(
            exchange_kernel,
            out_shape=[
                pltpu.VMEM((groups, n, full, SEQS * pos, LANE), jnp.float32),
                pltpu.VMEM((groups, n, SEQS, LANE), jnp.float32),
                pltpu.VMEM((groups - 1, pos, SEQS, vocab), jnp.float32),
                pltpu.VMEM((pos, seq_dev), jnp.float32),
            ],
            in_specs=[in_smem, in_hbm, in_hbm, in_hbm],
            out_specs=[in_vmem] * 4,
            scratch_shapes=[
                pltpu.VMEM((n * SEQS, pos, depth), jnp.bfloat16),
                pltpu.VMEM((rows, depth), jnp.bfloat16),
                pltpu.VMEM((SLOTS, TILE, depth), jnp.bfloat16),
                pltpu.VMEM((TILE // LANE, rows, LANE), jnp.float32),
                pltpu.VMEM((n_tiles, TILE // LANE, rows, LANE), jnp.float32),
                pltpu.VMEM((groups, n, SEQS, LANE), jnp.float32),
                pltpu.VMEM((draft, SEQS, vocab), jnp.float32),
                dma((n,)),
                dma((SLOTS,)),
                dma((draft,)),
                dma((n_tiles,)),
                dma((groups, n - 1)),
                dma((n - 1,)),
                dma((groups, n - 1)),
            ],
            compiler_params=pltpu.CompilerParams(collective_id=0, has_side_effects=True, vmem_limit_bytes=VMEM_A * MIB),
            cost_estimate=pl.CostEstimate(flops=2 * batch * pos * depth * shard, bytes_accessed=2 * shard * depth, transcendentals=0),
            name="logits_exchange",
        )(x_t, hidden, w_shard.T, q_hbm)

        res, bonus, acc, expd = pl.pallas_call(
            output_kernel,
            out_shape=[
                jax.ShapeDtypeStruct((draft, seq_dev, vocab), jnp.float32),
                jax.ShapeDtypeStruct((seq_dev, vocab), jnp.float32),
                jax.ShapeDtypeStruct((draft, seq_dev), jnp.float32),
                jax.ShapeDtypeStruct((1, seq_dev), jnp.float32),
            ],
            in_specs=[in_smem, in_vmem, in_vmem, in_vmem, in_vmem, in_hbm],
            out_specs=[in_hbm, in_hbm, in_vmem, in_vmem],
            scratch_shapes=[
                pltpu.VMEM((pos, SEQS, vocab), jnp.float32),
                pltpu.VMEM((draft, SEQS, vocab), jnp.float32),
                dma((draft,)),
                dma((groups, pos)),
            ],
            compiler_params=pltpu.CompilerParams(vmem_limit_bytes=VMEM_B * MIB),
            name="write_outputs",
        )(x_t, *(pltpu.with_memory_space_constraint(a, pltpu.VMEM) for a in (recv, edge, done, part)), q_hbm)
        return acc.T, expd.reshape(seq_dev), res.transpose(1, 0, 2), bonus

    return jax.shard_map(local_step, mesh=mesh,
                         in_specs=(P("dp", None, None), P(None, "tp"), P(("dp", "tp"), None, None), P("dp", None)),
                         out_specs=(P(("dp", "tp"), None), P(("dp", "tp")), P(("dp", "tp"), None, None), P(("dp", "tp"), None)),
                         check_vma=False)
```

```python
import jax
import jax.numpy as jnp
from jax import lax
from jax.experimental import pallas as pl
from jax.experimental.pallas import tpu as pltpu
from jax.sharding import PartitionSpec as P

INV_TEMP = 1.25
MESH = pl.DeviceIdType.MESH
LANE = 128
TILE = 256
SEQS = 8
SLOTS = 3
ORDER = (6, 2, 4, 7, 3, 5, 1)
CHAINS = 4
WIDE = 25
MIB = 1024 * 1024
VMEM_A = 32
VMEM_B = 32


def peer_of(me, k):
    d = me
    for bit in (1, 2, 4):
        if k & bit:
            d = d + bit * (1 - 2 * ((me // bit) % 2))
    return d


def lanes(g):
    return pl.ds(pl.multiple_of(g * LANE, LANE), LANE)


def chunk(i):
    return pl.ds(pl.multiple_of(i * (WIDE * LANE), LANE), WIDE * LANE)


def chained(op, n, unroll, term, parts):
    def body(c, parts):
        return (*parts[1:], op(parts[0], term(c)))

    return lax.fori_loop(0, n, body, parts, unroll=unroll)


def across(op, reduce, parts):
    v = parts[0]
    for p in parts[1:]:
        v = op(v, p)
    return reduce(v, axis=1, keepdims=True)


def softmax_rows(tile, edge, put, n_src, full, tail, seqs):
    shard = full * LANE + tail
    shape = (seqs, LANE)
    lane = lax.broadcasted_iota(jnp.int32, shape, 1)
    parts = (tile(0, 0),) * CHAINS
    for s in range(n_src):
        parts = chained(jnp.maximum, full, full, lambda c: tile(s, c), parts)
        parts = (*parts[1:], jnp.maximum(parts[0], jnp.where(lane < tail, edge(s), -jnp.inf)))
    peak = jnp.broadcast_to(across(jnp.maximum, jnp.max, parts), shape)
    pend = tile(0, 0) * 0.0
    parts = (pend,) * CHAINS
    for s in range(n_src):
        off = s * shard % LANE
        base = s * shard // LANE

        def place(i, e, pend):
            r = pltpu.roll(e, off, 1) if off else e
            v = jnp.where(lane < off, pend, r) if off else r
            return r, v

        def body(c, carry):
            pend, *parts = carry
            e = jnp.exp(tile(s, c) - peak)
            r, v = place(base + c, e, pend)
            put(base + c, v)
            return (r, *parts[1:], parts[0] + e)

        pend, *parts = lax.fori_loop(0, full, body, (pend, *parts), unroll=full)
        e = jnp.where(lane < tail, jnp.exp(edge(s) - peak), 0.0)
        parts = [*parts[1:], parts[0] + e]
        _, pend = place(base + full, e, pend)
        if off + tail == LANE:
            put(base + full, pend)
    return 1.0 / across(jnp.add, jnp.sum, parts)


def fold(op, parts, wide):
    for k in range(0, wide.shape[1], LANE):
        parts = (*parts[1:], op(parts[0], wide[:, k:k + LANE]))
    return parts


def finish_bonus(get, put, inv, n_g):
    def body(i, carry):
        put(i, get(i) * inv)
        return carry

    lax.fori_loop(0, n_g // WIDE, body, 0)


def excess_rows(get, q_tile, inv, n_g):
    zero = get(0)[:, :LANE] * 0.0
    parts = lax.fori_loop(
        0, n_g // WIDE, lambda i, parts: fold(jnp.add, parts, jnp.maximum(get(i) * inv - q_tile(i), 0.0)), (zero,) * CHAINS)
    return 1.0 / across(jnp.add, jnp.sum, parts)


def excess_rows_with_picks(get, q_tile, token, inv, n_g):
    shape = (inv.shape[0], LANE)
    lane = lax.broadcasted_iota(jnp.int32, shape, 1)
    row = lax.broadcasted_iota(jnp.int32, shape, 0)
    x = jnp.zeros(shape, jnp.int32)
    for b in range(shape[0]):
        x = jnp.where(row == b, token(b), x)
    x = x - lane

    def body(i, carry):
        p_pick, q_pick, *parts = carry
        p, q = get(i) * inv, q_tile(i)
        for k in range(WIDE):
            hit = x == (i * WIDE + k) * LANE
            p_pick = jnp.where(hit, p[:, k * LANE:(k + 1) * LANE], p_pick)
            q_pick = jnp.where(hit, q[:, k * LANE:(k + 1) * LANE], q_pick)
        return (p_pick, q_pick, *fold(jnp.add, tuple(parts), jnp.maximum(p - q, 0.0)))

    zero = get(0)[:, :LANE] * 0.0
    p_pick, q_pick, *parts = lax.fori_loop(0, n_g // WIDE, body, (zero,) * (CHAINS + 2))
    return 1.0 / across(jnp.add, jnp.sum, parts), accept_column(p_pick, q_pick)


def accept_column(p_pick, q_pick):
    return jnp.minimum(1.0, jnp.sum(p_pick, axis=1, keepdims=True) / jnp.sum(q_pick, axis=1, keepdims=True))


def picks_at(get_at, q_at, token, inv):
    shape = (inv.shape[0], LANE)
    lane = lax.broadcasted_iota(jnp.int32, shape, 1)
    row = lax.broadcasted_iota(jnp.int32, shape, 0)
    p_pick = jnp.zeros(shape, jnp.float32)
    q_pick = jnp.zeros(shape, jnp.float32)
    for b in range(shape[0]):
        x = token(b)
        at = pl.multiple_of((x // LANE) * LANE, LANE)
        hit = (row == b) & (lane == x - at)
        p_pick = jnp.where(hit, get_at(at) * inv, p_pick)
        q_pick = jnp.where(hit, q_at(at), q_pick)
    return accept_column(p_pick, q_pick)


def residual_rows(get, put, q_tile, inv, scale, n_g):
    def body(i, carry):
        put(i, jnp.maximum(get(i) * inv - q_tile(i), 0.0) * scale)
        return carry

    lax.fori_loop(0, n_g // WIDE, body, 0)


def to_lanes(col, first, n_out):
    seqs = col.shape[0]
    wide = lax.broadcasted_iota(jnp.int32, (seqs, n_out), 1)
    deep = lax.broadcasted_iota(jnp.int32, (seqs, n_out), 0)
    return jnp.sum(jnp.where(wide == deep + first, jnp.broadcast_to(col, (seqs, n_out)), 0.0), axis=0, keepdims=True)


def prefixes(accepts):
    run, expected = accepts[0], accepts[0]
    for a in accepts[1:]:
        run = run * a
        expected = expected + run
    return expected


def exchange_kernel(x_ref, h_ref, w_ref, q_ref, recv_ref, edge_ref, done_ref, acc_ref, stage, h_buf, w_buf, z_buf, send_buf, edge_buf, q_buf,
                    h_sem, w_sem, q_sem, send_sem, recv_sem, edge_send, edge_recv):
    me = lax.axis_index("tp")
    vocab, depth = w_ref.shape
    groups, n_dev = recv_ref.shape[:2]
    seqs = stage.shape[0] // n_dev
    pos = stage.shape[1]
    draft = pos - 1
    seg = seqs * pos
    per_dev = groups * seqs
    n_tiles = pl.cdiv(vocab, TILE)
    last = vocab - (n_tiles - 1) * TILE
    lt = TILE // LANE
    full = vocab // LANE
    tail = vocab - full * LANE
    n_steps = groups * n_tiles
    lane = lax.broadcasted_iota(jnp.int32, (seqs, LANE), 1)

    def w_copy(u, size):
        slot = lax.rem(u, SLOTS)
        t = lax.rem(u, n_tiles)
        return pltpu.make_async_copy(w_ref.at[pl.ds(pl.multiple_of(t * TILE, TILE), size)], w_buf.at[slot, pl.ds(0, size)], w_sem.at[slot])

    def on_tile(u, act):
        t = lax.rem(u, n_tiles)

        @pl.when(t < n_tiles - 1)
        def _():
            act(w_copy(u, TILE))

        @pl.when(t == n_tiles - 1)
        def _():
            act(w_copy(u, last))

    def h_copy(g, d):
        src = h_ref.at[pl.ds(d * per_dev + g * seqs, seqs)]
        return pltpu.make_async_copy(src, stage.at[pl.ds(d * seqs, seqs)], h_sem.at[d])

    def h_start(g):
        for d in range(n_dev):
            h_copy(g, d).start()

    def relayout(g):
        for d in range(n_dev):
            h_copy(g, d).wait()

            def cols(c, carry):
                at = pl.ds(pl.multiple_of(c * LANE, LANE), LANE)
                h_buf[pl.ds(d * seg, seg), at] = stage[pl.ds(d * seqs, seqs), :, at].reshape(seg, LANE)
                return carry

            lax.fori_loop(0, depth // LANE, cols, 0, unroll=8)

    def q_copy(g, j):
        return pltpu.make_async_copy(q_ref.at[j, pl.ds(pl.multiple_of(g * seqs, seqs), seqs)], q_buf.at[j], q_sem.at[j])

    h_start(0)
    w_copy(0, TILE).start()
    w_copy(1, TILE).start()

    barrier = pltpu.get_barrier_semaphore()
    for k in range(1, n_dev):
        pl.semaphore_signal(barrier, inc=1, device_id={"tp": peer_of(me, k)}, device_id_type=MESH)

    acc_ref[...] = jnp.zeros_like(acc_ref)
    relayout(0)
    h_start(1)
    pl.semaphore_wait(barrier, n_dev - 1)

    def send(g, t, width):
        for c in range(width):
            recv_ref[g, me, t * lt + c] = send_buf[t, c, pl.ds(pl.multiple_of(me * seg, seg), seg), :]
        for k in ORDER:
            d = peer_of(me, k)
            pltpu.make_async_remote_copy(
                src_ref=send_buf.at[t, pl.ds(0, width), pl.ds(pl.multiple_of(d * seg, seg), seg)],
                dst_ref=recv_ref.at[g, me, pl.ds(t * lt, width)],
                send_sem=send_sem.at[t],
                recv_sem=recv_sem.at[g, k - 1],
                device_id={"tp": d},
                device_id_type=MESH,
            ).start()

    def wait_sent(t, width):
        ref = send_buf.at[t, pl.ds(0, width), pl.ds(0, (n_dev - 1) * seg)]
        pltpu.make_async_remote_copy(
            src_ref=ref, dst_ref=ref, send_sem=send_sem.at[t], recv_sem=recv_sem.at[0, 0],
            device_id={"tp": peer_of(me, 1)}, device_id_type=MESH,
        ).wait_send()

    def send_edge(g):
        for d in range(n_dev):
            packed = z_buf[1, pl.ds(d * seg, seqs, stride=pos), :]
            for j in range(1, pos):
                v = pltpu.roll(z_buf[1, pl.ds(d * seg + j, seqs, stride=pos), :], j * tail, 1)
                packed = jnp.where(lane < j * tail, packed, v)
            edge_buf[g, d] = packed
        edge_ref[g, me] = edge_buf[g, me]
        for k in ORDER:
            d = peer_of(me, k)
            pltpu.make_async_remote_copy(
                src_ref=edge_buf.at[g, d],
                dst_ref=edge_ref.at[g, me],
                send_sem=edge_send.at[k - 1],
                recv_sem=edge_recv.at[g, k - 1],
                device_id={"tp": d},
                device_id_type=MESH,
            ).start()

    rest = full - (n_tiles - 1) * lt

    def step(u, carry):
        g = u // n_tiles
        t = lax.rem(u, n_tiles)
        slot = lax.rem(u, SLOTS)

        @pl.when((t == 0) & (g > 0))
        def _():
            relayout(g)

            @pl.when(g + 1 < groups)
            def _():
                h_start(g + 1)

        on_tile(u, lambda c: c.wait())

        @pl.when(u + 2 < n_steps)
        def _():
            on_tile(u + 2, lambda c: c.start())

        z = lax.dot_general(h_buf[...], w_buf[slot], (((1,), (1,)), ((), ())), preferred_element_type=jnp.float32) * INV_TEMP
        for c in range(lt):
            z_buf[c] = z[:, c * LANE:(c + 1) * LANE]

        @pl.when((g > 0) & (t < n_tiles - 1))
        def _():
            wait_sent(t, lt)

        @pl.when((g > 0) & (t == n_tiles - 1))
        def _():
            wait_sent(t, rest)

        for c in range(lt):
            for d in range(n_dev):
                for j in range(pos):
                    send_buf[t, c, pl.ds(d * seg + j * seqs, seqs), :] = z_buf[c, pl.ds(d * seg + j, seqs, stride=pos), :]

        @pl.when(t < n_tiles - 1)
        def _():
            send(g, t, lt)

        @pl.when(t == n_tiles - 1)
        def _():
            send(g, t, rest)
            send_edge(g)

        return carry

    lax.fori_loop(0, n_steps, step, 0)

    def wait_group(g):
        for k in ORDER:
            d = peer_of(me, k)
            for ref, ss, rs in ((recv_ref, edge_send, recv_sem), (edge_ref, edge_send, edge_recv)):
                pltpu.make_async_remote_copy(
                    src_ref=ref.at[g, d], dst_ref=ref.at[g, d], send_sem=ss.at[k - 1], recv_sem=rs.at[g, k - 1],
                    device_id={"tp": d}, device_id_type=MESH,
                ).wait_recv()

    for j in range(draft):
        q_copy(0, j).start()

    def finish(g, carry):
        wait_group(g)
        accepts = []
        for j in range(pos):
            def tile(s, c):
                return recv_ref[g, s, c, pl.ds(j * seqs, seqs), :]

            def edge(s):
                v = edge_ref[g, s]
                return pltpu.roll(v, LANE - j * tail, 1) if j else v

            def put(i, v):
                done_ref[g, j, :, lanes(i)] = v

            def get(i):
                return done_ref[g, j, :, chunk(i)]

            def put_wide(i, v):
                done_ref[g, j, :, chunk(i)] = v

            n_g = done_ref.shape[3] // LANE
            inv = softmax_rows(tile, edge, put, n_dev, full, tail, seqs)
            if j == draft:
                finish_bonus(get, put_wide, inv, n_g)
                continue
            q_copy(g, j).wait()
            def q_tile(i):
                return q_buf[j, :, chunk(i)]

            scale, accept = excess_rows_with_picks(get, q_tile, lambda b: x_ref[j, me * per_dev + g * seqs + b], inv, n_g)
            accepts.append(accept)
            residual_rows(get, put_wide, q_tile, inv, scale, n_g)

            @pl.when(g + 2 < groups)
            def _():
                q_copy(g + 1, j).start()

        for j in range(draft):
            acc_ref[j:j + 1, :] += to_lanes(accepts[j], g * seqs, per_dev)
        acc_ref[draft:pos, :] += to_lanes(prefixes(accepts), g * seqs, per_dev)
        return carry

    lax.fori_loop(0, groups - 1, finish, 0)
    wait_group(groups - 1)

    for t in range(n_tiles):
        wait_sent(t, lt if t < n_tiles - 1 else rest)
    for k in ORDER:
        d = peer_of(me, k)
        ref = edge_ref.at[:, d]
        pltpu.make_async_remote_copy(
            src_ref=ref, dst_ref=ref, send_sem=edge_send.at[k - 1], recv_sem=edge_recv.at[0, k - 1],
            device_id={"tp": d}, device_id_type=MESH,
        ).wait_send()


def output_kernel(x_ref, recv_ref, edge_ref, done_ref, part_ref, q_ref, res_ref, bonus_ref, acc_ref, exp_ref, row_buf, q_buf, q_sem, out_sem):
    me = lax.axis_index("tp")
    groups, n_dev, full = recv_ref.shape[:3]
    seqs = edge_ref.shape[2]
    pos = done_ref.shape[1]
    draft = pos - 1
    vocab = done_ref.shape[3]
    n_g = vocab // LANE
    tail = vocab // n_dev - full * LANE
    per_dev = groups * seqs
    g_last = groups - 1

    def q_copy(j):
        return pltpu.make_async_copy(q_ref.at[j, pl.ds(g_last * seqs, seqs)], q_buf.at[j], q_sem.at[j])

    def out(g, j, src):
        dst = bonus_ref if j == draft else res_ref.at[j]
        return pltpu.make_async_copy(src, dst.at[pl.ds(g * seqs, seqs)], out_sem.at[g, j])

    for j in range(draft):
        q_copy(j).start()
    for g in range(g_last):
        for j in range(pos):
            out(g, j, done_ref.at[g, j]).start()

    accepts = []
    for j in (draft, *range(draft)):
        def tile(s, c):
            return recv_ref[g_last, s, c, pl.ds(j * seqs, seqs), :]

        def edge(s):
            v = edge_ref[g_last, s]
            return pltpu.roll(v, LANE - j * tail, 1) if j else v

        def put(i, v):
            row_buf[j, :, lanes(i)] = v

        def get(i):
            return row_buf[j, :, chunk(i)]

        def put_wide(i, v):
            row_buf[j, :, chunk(i)] = v

        inv = softmax_rows(tile, edge, put, n_dev, full, tail, seqs)
        if j == draft:
            finish_bonus(get, put_wide, inv, n_g)
        else:
            q_copy(j).wait()
            def q_tile(i):
                return q_buf[j, :, chunk(i)]

            accepts.append(picks_at(
                lambda at: row_buf[j, :, pl.ds(at, LANE)], lambda at: q_buf[j, :, pl.ds(at, LANE)],
                lambda b: x_ref[j, me * per_dev + g_last * seqs + b], inv))
            residual_rows(get, put_wide, q_tile, inv, excess_rows(get, q_tile, inv, n_g), n_g)
        out(g_last, j, row_buf.at[j]).start()

    for j in range(draft):
        acc_ref[j:j + 1, :] = part_ref[j:j + 1, :] + to_lanes(accepts[j], g_last * seqs, per_dev)
    exp_ref[...] = part_ref[draft:pos, :] + to_lanes(prefixes(accepts), g_last * seqs, per_dev)
    for g in range(groups):
        for j in range(pos):
            out(g, j, row_buf.at[j]).wait()


def solution(mesh):
    n = mesh.shape["tp"]

    def local_step(hidden, w_shard, q_rows, x_group):
        seq_dev, draft, vocab = q_rows.shape
        batch, pos, depth = hidden.shape
        shard = w_shard.shape[1]
        n_tiles = pl.cdiv(shard, TILE)
        groups = seq_dev // SEQS
        rows = n * SEQS * pos
        full = shard // LANE
        dma = pltpu.SemaphoreType.DMA
        in_hbm = pl.BlockSpec(memory_space=pltpu.HBM)
        in_vmem = pl.BlockSpec(memory_space=pltpu.VMEM)
        in_smem = pl.BlockSpec(memory_space=pltpu.SMEM)
        x_t = x_group.T
        q_hbm = pltpu.with_memory_space_constraint(q_rows.transpose(1, 0, 2), pltpu.HBM)

        recv, edge, done, part = pl.pallas_call(
            exchange_kernel,
            out_shape=[
                pltpu.VMEM((groups, n, full, SEQS * pos, LANE), jnp.float32),
                pltpu.VMEM((groups, n, SEQS, LANE), jnp.float32),
                pltpu.VMEM((groups - 1, pos, SEQS, vocab), jnp.float32),
                pltpu.VMEM((pos, seq_dev), jnp.float32),
            ],
            in_specs=[in_smem, in_hbm, in_hbm, in_hbm],
            out_specs=[in_vmem] * 4,
            scratch_shapes=[
                pltpu.VMEM((n * SEQS, pos, depth), jnp.bfloat16),
                pltpu.VMEM((rows, depth), jnp.bfloat16),
                pltpu.VMEM((SLOTS, TILE, depth), jnp.bfloat16),
                pltpu.VMEM((TILE // LANE, rows, LANE), jnp.float32),
                pltpu.VMEM((n_tiles, TILE // LANE, rows, LANE), jnp.float32),
                pltpu.VMEM((groups, n, SEQS, LANE), jnp.float32),
                pltpu.VMEM((draft, SEQS, vocab), jnp.float32),
                dma((n,)),
                dma((SLOTS,)),
                dma((draft,)),
                dma((n_tiles,)),
                dma((groups, n - 1)),
                dma((n - 1,)),
                dma((groups, n - 1)),
            ],
            compiler_params=pltpu.CompilerParams(collective_id=0, has_side_effects=True, vmem_limit_bytes=VMEM_A * MIB),
            cost_estimate=pl.CostEstimate(flops=2 * batch * pos * depth * shard, bytes_accessed=2 * shard * depth, transcendentals=0),
            name="logits_exchange",
        )(x_t, hidden, w_shard.T, q_hbm)

        res, bonus, acc, expd = pl.pallas_call(
            output_kernel,
            out_shape=[
                jax.ShapeDtypeStruct((draft, seq_dev, vocab), jnp.float32),
                jax.ShapeDtypeStruct((seq_dev, vocab), jnp.float32),
                jax.ShapeDtypeStruct((draft, seq_dev), jnp.float32),
                jax.ShapeDtypeStruct((1, seq_dev), jnp.float32),
            ],
            in_specs=[in_smem, in_vmem, in_vmem, in_vmem, in_vmem, in_hbm],
            out_specs=[in_hbm, in_hbm, in_vmem, in_vmem],
            scratch_shapes=[
                pltpu.VMEM((pos, SEQS, vocab), jnp.float32),
                pltpu.VMEM((draft, SEQS, vocab), jnp.float32),
                dma((draft,)),
                dma((groups, pos)),
            ],
            compiler_params=pltpu.CompilerParams(vmem_limit_bytes=VMEM_B * MIB),
            name="write_outputs",
        )(x_t, *(pltpu.with_memory_space_constraint(a, pltpu.VMEM) for a in (recv, edge, done, part)), q_hbm)
        return acc.T, expd.reshape(seq_dev), res.transpose(1, 0, 2), bonus

    return jax.shard_map(local_step, mesh=mesh,
                         in_specs=(P("dp", None, None), P(None, "tp"), P(("dp", "tp"), None, None), P("dp", None)),
                         out_specs=(P(("dp", "tp"), None), P(("dp", "tp")), P(("dp", "tp"), None, None), P(("dp", "tp"), None)),
                         check_vma=False)
```

```python
import jax
import jax.numpy as jnp
from jax import lax
from jax.experimental import pallas as pl
from jax.experimental.pallas import tpu as pltpu
from jax.sharding import PartitionSpec as P

INV_TEMP = 1.25
MESH = pl.DeviceIdType.MESH
LANE = 128
TILE = 256
SEQS = 8
SLOTS = 3
ORDER = (6, 2, 4, 7, 3, 5, 1)
H_PART = 8
CHAINS = 4
WIDE = 25
MIB = 1024 * 1024
VMEM_A = 29
VMEM_B = 29


def peer_of(me, k):
    d = me
    for bit in (1, 2, 4):
        if k & bit:
            d = d + bit * (1 - 2 * ((me // bit) % 2))
    return d


def lanes(g):
    return pl.ds(pl.multiple_of(g * LANE, LANE), LANE)


def chunk(i):
    return pl.ds(pl.multiple_of(i * (WIDE * LANE), LANE), WIDE * LANE)


def chained(op, n, unroll, term, parts):
    def body(c, parts):
        return (*parts[1:], op(parts[0], term(c)))

    return lax.fori_loop(0, n, body, parts, unroll=unroll)


def across(op, reduce, parts):
    v = parts[0]
    for p in parts[1:]:
        v = op(v, p)
    return reduce(v, axis=1, keepdims=True)


def softmax_rows(tile, edge, put, n_src, full, tail, seqs):
    shard = full * LANE + tail
    shape = (seqs, LANE)
    lane = lax.broadcasted_iota(jnp.int32, shape, 1)
    parts = (tile(0, 0),) * CHAINS
    for s in range(n_src):
        parts = chained(jnp.maximum, full, full, lambda c: tile(s, c), parts)
        parts = (*parts[1:], jnp.maximum(parts[0], jnp.where(lane < tail, edge(s), -jnp.inf)))
    peak = jnp.broadcast_to(across(jnp.maximum, jnp.max, parts), shape)
    pend = tile(0, 0) * 0.0
    parts = (pend,) * CHAINS
    for s in range(n_src):
        off = s * shard % LANE
        base = s * shard // LANE

        def place(i, e, pend):
            r = pltpu.roll(e, off, 1) if off else e
            v = jnp.where(lane < off, pend, r) if off else r
            return r, v

        def body(c, carry):
            pend, *parts = carry
            e = jnp.exp(tile(s, c) - peak)
            r, v = place(base + c, e, pend)
            put(base + c, v)
            return (r, *parts[1:], parts[0] + e)

        pend, *parts = lax.fori_loop(0, full, body, (pend, *parts), unroll=full)
        e = jnp.where(lane < tail, jnp.exp(edge(s) - peak), 0.0)
        parts = [*parts[1:], parts[0] + e]
        _, pend = place(base + full, e, pend)
        if off + tail == LANE:
            put(base + full, pend)
    return 1.0 / across(jnp.add, jnp.sum, parts)


def fold(op, parts, wide):
    for k in range(0, wide.shape[1], LANE):
        parts = (*parts[1:], op(parts[0], wide[:, k:k + LANE]))
    return parts


def finish_bonus(get, put, inv, n_g):
    def body(i, carry):
        put(i, get(i) * inv)
        return carry

    lax.fori_loop(0, n_g // WIDE, body, 0)


def excess_rows(get, q_tile, inv, n_g):
    zero = get(0)[:, :LANE] * 0.0
    parts = lax.fori_loop(
        0, n_g // WIDE, lambda i, parts: fold(jnp.add, parts, jnp.maximum(get(i) * inv - q_tile(i), 0.0)), (zero,) * CHAINS)
    return 1.0 / across(jnp.add, jnp.sum, parts)


def excess_rows_with_picks(get, q_tile, token, inv, n_g):
    shape = (inv.shape[0], LANE)
    lane = lax.broadcasted_iota(jnp.int32, shape, 1)
    row = lax.broadcasted_iota(jnp.int32, shape, 0)
    x = jnp.zeros(shape, jnp.int32)
    for b in range(shape[0]):
        x = jnp.where(row == b, token(b), x)
    x = x - lane

    def body(i, carry):
        p_pick, q_pick, *parts = carry
        p, q = get(i) * inv, q_tile(i)
        for k in range(WIDE):
            hit = x == (i * WIDE + k) * LANE
            p_pick = jnp.where(hit, p[:, k * LANE:(k + 1) * LANE], p_pick)
            q_pick = jnp.where(hit, q[:, k * LANE:(k + 1) * LANE], q_pick)
        return (p_pick, q_pick, *fold(jnp.add, tuple(parts), jnp.maximum(p - q, 0.0)))

    zero = get(0)[:, :LANE] * 0.0
    p_pick, q_pick, *parts = lax.fori_loop(0, n_g // WIDE, body, (zero,) * (CHAINS + 2))
    return 1.0 / across(jnp.add, jnp.sum, parts), accept_column(p_pick, q_pick)


def accept_column(p_pick, q_pick):
    return jnp.minimum(1.0, jnp.sum(p_pick, axis=1, keepdims=True) / jnp.sum(q_pick, axis=1, keepdims=True))


def picks_at(get_at, q_at, token, inv):
    shape = (inv.shape[0], LANE)
    lane = lax.broadcasted_iota(jnp.int32, shape, 1)
    row = lax.broadcasted_iota(jnp.int32, shape, 0)
    p_pick = jnp.zeros(shape, jnp.float32)
    q_pick = jnp.zeros(shape, jnp.float32)
    for b in range(shape[0]):
        x = token(b)
        at = pl.multiple_of((x // LANE) * LANE, LANE)
        hit = (row == b) & (lane == x - at)
        p_pick = jnp.where(hit, get_at(at) * inv, p_pick)
        q_pick = jnp.where(hit, q_at(at), q_pick)
    return accept_column(p_pick, q_pick)


def residual_rows(get, put, q_tile, inv, scale, n_g):
    def body(i, carry):
        put(i, jnp.maximum(get(i) * inv - q_tile(i), 0.0) * scale)
        return carry

    lax.fori_loop(0, n_g // WIDE, body, 0)


def to_lanes(col, first, n_out):
    seqs = col.shape[0]
    wide = lax.broadcasted_iota(jnp.int32, (seqs, n_out), 1)
    deep = lax.broadcasted_iota(jnp.int32, (seqs, n_out), 0)
    return jnp.sum(jnp.where(wide == deep + first, jnp.broadcast_to(col, (seqs, n_out)), 0.0), axis=0, keepdims=True)


def prefixes(accepts):
    run, expected = accepts[0], accepts[0]
    for a in accepts[1:]:
        run = run * a
        expected = expected + run
    return expected


def exchange_kernel(x_ref, h_ref, w_ref, q_ref, recv_ref, edge_ref, done_ref, acc_ref, q_buf, stage, h_buf, w_buf, z_buf, send_buf, edge_buf,
                    h_sem, w_sem, q_sem, send_sem, recv_sem, edge_send, edge_recv):
    me = lax.axis_index("tp")
    vocab, depth = w_ref.shape
    groups, n_dev = recv_ref.shape[:2]
    seqs, pos = stage.shape[2:4]
    draft = pos - 1
    seg = seqs * pos
    per_dev = groups * seqs
    n_tiles = pl.cdiv(vocab, TILE)
    last = vocab - (n_tiles - 1) * TILE
    lt = TILE // LANE
    full = vocab // LANE
    tail = vocab - full * LANE
    n_steps = groups * n_tiles
    lane = lax.broadcasted_iota(jnp.int32, (seqs, LANE), 1)

    def w_copy(u, size):
        slot = lax.rem(u, SLOTS)
        t = lax.rem(u, n_tiles)
        return pltpu.make_async_copy(w_ref.at[pl.ds(pl.multiple_of(t * TILE, TILE), size)], w_buf.at[slot, pl.ds(0, size)], w_sem.at[slot])

    def on_tile(u, act):
        t = lax.rem(u, n_tiles)

        @pl.when(t < n_tiles - 1)
        def _():
            act(w_copy(u, TILE))

        @pl.when(t == n_tiles - 1)
        def _():
            act(w_copy(u, last))

    def h_copy(g, c):
        src = h_ref.at[:, pl.ds(pl.multiple_of(g * seqs, seqs), seqs), :, lanes(c)]
        return pltpu.make_async_copy(src, stage.at[c], h_sem.at[c // H_PART])

    def h_start(g):
        for c in range(depth // LANE):
            h_copy(g, c).start()

    def relayout(g):
        flat = stage.reshape(depth // LANE, n_dev * seg, LANE)

        def part(i, carry):
            part_ref = stage.at[pl.ds(i * H_PART, H_PART)]
            pltpu.make_async_copy(part_ref, part_ref, h_sem.at[i]).wait()

            def cols(c, carry):
                h_buf[:, lanes(i * H_PART + c)] = flat[i * H_PART + c]
                return carry

            return lax.fori_loop(0, H_PART, cols, carry, unroll=True)

        lax.fori_loop(0, depth // LANE // H_PART, part, 0)

    def q_copy(g, j):
        return pltpu.make_async_copy(q_ref.at[j, pl.ds(pl.multiple_of(g * seqs, seqs), seqs)], q_buf.at[j], q_sem.at[j])

    h_start(0)
    w_copy(0, TILE).start()
    w_copy(1, TILE).start()

    barrier = pltpu.get_barrier_semaphore()
    for k in range(1, n_dev):
        pl.semaphore_signal(barrier, inc=1, device_id={"tp": peer_of(me, k)}, device_id_type=MESH)

    acc_ref[...] = jnp.zeros_like(acc_ref)
    relayout(0)
    h_start(1)
    pl.semaphore_wait(barrier, n_dev - 1)

    def send(g, t, width):
        for c in range(width):
            recv_ref[g, me, t * lt + c] = send_buf[t, c, pl.ds(pl.multiple_of(me * seg, seg), seg), :]
        for k in ORDER:
            d = peer_of(me, k)
            pltpu.make_async_remote_copy(
                src_ref=send_buf.at[t, pl.ds(0, width), pl.ds(pl.multiple_of(d * seg, seg), seg)],
                dst_ref=recv_ref.at[g, me, pl.ds(t * lt, width)],
                send_sem=send_sem.at[t],
                recv_sem=recv_sem.at[g, k - 1],
                device_id={"tp": d},
                device_id_type=MESH,
            ).start()

    def wait_sent(t, width):
        ref = send_buf.at[t, pl.ds(0, width), pl.ds(0, (n_dev - 1) * seg)]
        pltpu.make_async_remote_copy(
            src_ref=ref, dst_ref=ref, send_sem=send_sem.at[t], recv_sem=recv_sem.at[0, 0],
            device_id={"tp": peer_of(me, 1)}, device_id_type=MESH,
        ).wait_send()

    def send_edge(g):
        for d in range(n_dev):
            packed = z_buf[1, pl.ds(d * seg, seqs, stride=pos), :]
            for j in range(1, pos):
                v = pltpu.roll(z_buf[1, pl.ds(d * seg + j, seqs, stride=pos), :], j * tail, 1)
                packed = jnp.where(lane < j * tail, packed, v)
            edge_buf[g, d] = packed
        edge_ref[g, me] = edge_buf[g, me]
        for k in ORDER:
            d = peer_of(me, k)
            pltpu.make_async_remote_copy(
                src_ref=edge_buf.at[g, d],
                dst_ref=edge_ref.at[g, me],
                send_sem=edge_send.at[k - 1],
                recv_sem=edge_recv.at[g, k - 1],
                device_id={"tp": d},
                device_id_type=MESH,
            ).start()

    rest = full - (n_tiles - 1) * lt

    def step(u, carry):
        g = u // n_tiles
        t = lax.rem(u, n_tiles)
        slot = lax.rem(u, SLOTS)

        @pl.when((t == 0) & (g > 0))
        def _():
            relayout(g)

            @pl.when(g + 1 < groups)
            def _():
                h_start(g + 1)

        on_tile(u, lambda c: c.wait())

        @pl.when(u + 2 < n_steps)
        def _():
            on_tile(u + 2, lambda c: c.start())

        z = lax.dot_general(h_buf[...], w_buf[slot], (((1,), (1,)), ((), ())), preferred_element_type=jnp.float32) * INV_TEMP
        for c in range(lt):
            z_buf[c] = z[:, c * LANE:(c + 1) * LANE]

        @pl.when((g > 0) & (t < n_tiles - 1))
        def _():
            wait_sent(t, lt)

        @pl.when((g > 0) & (t == n_tiles - 1))
        def _():
            wait_sent(t, rest)

        for c in range(lt):
            for d in range(n_dev):
                for j in range(pos):
                    send_buf[t, c, pl.ds(d * seg + j * seqs, seqs), :] = z_buf[c, pl.ds(d * seg + j, seqs, stride=pos), :]

        @pl.when(t < n_tiles - 1)
        def _():
            send(g, t, lt)

        @pl.when(t == n_tiles - 1)
        def _():
            send(g, t, rest)
            send_edge(g)

        return carry

    lax.fori_loop(0, n_steps, step, 0)

    def wait_group(g):
        for k in ORDER:
            d = peer_of(me, k)
            for ref, ss, rs in ((recv_ref, edge_send, recv_sem), (edge_ref, edge_send, edge_recv)):
                pltpu.make_async_remote_copy(
                    src_ref=ref.at[g, d], dst_ref=ref.at[g, d], send_sem=ss.at[k - 1], recv_sem=rs.at[g, k - 1],
                    device_id={"tp": d}, device_id_type=MESH,
                ).wait_recv()

    for j in range(draft):
        q_copy(0, j).start()

    def finish(g, carry):
        wait_group(g)
        accepts = []
        for j in range(pos):
            def tile(s, c):
                return recv_ref[g, s, c, pl.ds(j * seqs, seqs), :]

            def edge(s):
                v = edge_ref[g, s]
                return pltpu.roll(v, LANE - j * tail, 1) if j else v

            def put(i, v):
                done_ref[g, j, :, lanes(i)] = v

            def get(i):
                return done_ref[g, j, :, chunk(i)]

            def put_wide(i, v):
                done_ref[g, j, :, chunk(i)] = v

            n_g = done_ref.shape[3] // LANE
            inv = softmax_rows(tile, edge, put, n_dev, full, tail, seqs)
            if j == draft:
                finish_bonus(get, put_wide, inv, n_g)
                continue
            q_copy(g, j).wait()
            def q_tile(i):
                return q_buf[j, :, chunk(i)]

            scale, accept = excess_rows_with_picks(get, q_tile, lambda b: x_ref[j, me * per_dev + g * seqs + b], inv, n_g)
            accepts.append(accept)
            residual_rows(get, put_wide, q_tile, inv, scale, n_g)

            q_copy(g + 1, j).start()

        for j in range(draft):
            acc_ref[j:j + 1, :] += to_lanes(accepts[j], g * seqs, per_dev)
        acc_ref[draft:pos, :] += to_lanes(prefixes(accepts), g * seqs, per_dev)
        return carry

    lax.fori_loop(0, groups - 1, finish, 0)
    for j in range(draft):
        q_copy(groups - 1, j).wait()
    wait_group(groups - 1)

    for t in range(n_tiles):
        wait_sent(t, lt if t < n_tiles - 1 else rest)
    for k in ORDER:
        d = peer_of(me, k)
        ref = edge_ref.at[:, d]
        pltpu.make_async_remote_copy(
            src_ref=ref, dst_ref=ref, send_sem=edge_send.at[k - 1], recv_sem=edge_recv.at[0, k - 1],
            device_id={"tp": d}, device_id_type=MESH,
        ).wait_send()


def output_kernel(x_ref, recv_ref, edge_ref, done_ref, part_ref, q_buf, res_ref, bonus_ref, acc_ref, exp_ref, row_buf, out_sem):
    me = lax.axis_index("tp")
    groups, n_dev, full = recv_ref.shape[:3]
    seqs = edge_ref.shape[2]
    pos = done_ref.shape[1]
    draft = pos - 1
    vocab = done_ref.shape[3]
    n_g = vocab // LANE
    tail = vocab // n_dev - full * LANE
    per_dev = groups * seqs
    g_last = groups - 1

    def out(g, j, src):
        dst = bonus_ref if j == draft else res_ref.at[j]
        return pltpu.make_async_copy(src, dst.at[pl.ds(g * seqs, seqs)], out_sem.at[g, j])

    for g in range(g_last):
        for j in range(pos):
            out(g, j, done_ref.at[g, j]).start()

    accepts = []
    for j in (draft, *range(draft)):
        def tile(s, c):
            return recv_ref[g_last, s, c, pl.ds(j * seqs, seqs), :]

        def edge(s):
            v = edge_ref[g_last, s]
            return pltpu.roll(v, LANE - j * tail, 1) if j else v

        def put(i, v):
            row_buf[j, :, lanes(i)] = v

        def get(i):
            return row_buf[j, :, chunk(i)]

        def put_wide(i, v):
            row_buf[j, :, chunk(i)] = v

        inv = softmax_rows(tile, edge, put, n_dev, full, tail, seqs)
        if j == draft:
            finish_bonus(get, put_wide, inv, n_g)
        else:
            def q_tile(i):
                return q_buf[j, :, chunk(i)]

            accepts.append(picks_at(
                lambda at: row_buf[j, :, pl.ds(at, LANE)], lambda at: q_buf[j, :, pl.ds(at, LANE)],
                lambda b: x_ref[j, me * per_dev + g_last * seqs + b], inv))
            residual_rows(get, put_wide, q_tile, inv, excess_rows(get, q_tile, inv, n_g), n_g)
        out(g_last, j, row_buf.at[j]).start()

    for j in range(draft):
        acc_ref[j:j + 1, :] = part_ref[j:j + 1, :] + to_lanes(accepts[j], g_last * seqs, per_dev)
    exp_ref[...] = part_ref[draft:pos, :] + to_lanes(prefixes(accepts), g_last * seqs, per_dev)
    for g in range(groups):
        for j in range(pos):
            out(g, j, row_buf.at[j]).wait()


def solution(mesh):
    n = mesh.shape["tp"]

    def local_step(hidden, w_shard, q_rows, x_group):
        seq_dev, draft, vocab = q_rows.shape
        batch, pos, depth = hidden.shape
        shard = w_shard.shape[1]
        n_tiles = pl.cdiv(shard, TILE)
        groups = seq_dev // SEQS
        rows = n * SEQS * pos
        full = shard // LANE
        dma = pltpu.SemaphoreType.DMA
        in_hbm = pl.BlockSpec(memory_space=pltpu.HBM)
        in_vmem = pl.BlockSpec(memory_space=pltpu.VMEM)
        in_smem = pl.BlockSpec(memory_space=pltpu.SMEM)
        x_t = x_group.T
        q_hbm = pltpu.with_memory_space_constraint(q_rows.transpose(1, 0, 2), pltpu.HBM)

        recv, edge, done, part, q_last = pl.pallas_call(
            exchange_kernel,
            out_shape=[
                pltpu.VMEM((groups, n, full, SEQS * pos, LANE), jnp.float32),
                pltpu.VMEM((groups, n, SEQS, LANE), jnp.float32),
                pltpu.VMEM((groups - 1, pos, SEQS, vocab), jnp.float32),
                pltpu.VMEM((pos, seq_dev), jnp.float32),
                pltpu.VMEM((draft, SEQS, vocab), jnp.float32),
            ],
            in_specs=[in_smem, in_hbm, in_hbm, in_hbm],
            out_specs=[in_vmem] * 5,
            scratch_shapes=[
                pltpu.VMEM((depth // LANE, n, SEQS, pos, LANE), jnp.bfloat16),
                pltpu.VMEM((rows, depth), jnp.bfloat16),
                pltpu.VMEM((SLOTS, TILE, depth), jnp.bfloat16),
                pltpu.VMEM((TILE // LANE, rows, LANE), jnp.float32),
                pltpu.VMEM((n_tiles, TILE // LANE, rows, LANE), jnp.float32),
                pltpu.VMEM((groups, n, SEQS, LANE), jnp.float32),
                dma((depth // LANE // H_PART,)),
                dma((SLOTS,)),
                dma((draft,)),
                dma((n_tiles,)),
                dma((groups, n - 1)),
                dma((n - 1,)),
                dma((groups, n - 1)),
            ],
            compiler_params=pltpu.CompilerParams(collective_id=0, has_side_effects=True, vmem_limit_bytes=VMEM_A * MIB),
            cost_estimate=pl.CostEstimate(flops=2 * batch * pos * depth * shard, bytes_accessed=2 * shard * depth, transcendentals=0),
            name="logits_exchange",
        )(x_t, hidden.reshape(n, seq_dev, pos, depth), w_shard.T, q_hbm)

        res, bonus, acc, expd = pl.pallas_call(
            output_kernel,
            out_shape=[
                jax.ShapeDtypeStruct((draft, seq_dev, vocab), jnp.float32),
                jax.ShapeDtypeStruct((seq_dev, vocab), jnp.float32),
                jax.ShapeDtypeStruct((draft, seq_dev), jnp.float32),
                jax.ShapeDtypeStruct((1, seq_dev), jnp.float32),
            ],
            in_specs=[in_smem] + [in_vmem] * 5,
            out_specs=[in_hbm, in_hbm, in_vmem, in_vmem],
            scratch_shapes=[
                pltpu.VMEM((pos, SEQS, vocab), jnp.float32),
                dma((groups, pos)),
            ],
            compiler_params=pltpu.CompilerParams(vmem_limit_bytes=VMEM_B * MIB),
            name="write_outputs",
        )(x_t, *(pltpu.with_memory_space_constraint(a, pltpu.VMEM) for a in (recv, edge, done, part, q_last)))
        return acc.T, expd.reshape(seq_dev), res.transpose(1, 0, 2), bonus

    return jax.shard_map(local_step, mesh=mesh,
                         in_specs=(P("dp", None, None), P(None, "tp"), P(("dp", "tp"), None, None), P("dp", None)),
                         out_specs=(P(("dp", "tp"), None), P(("dp", "tp")), P(("dp", "tp"), None, None), P(("dp", "tp"), None)),
                         check_vma=False)
```

```python
import jax
import jax.numpy as jnp
from jax import lax
from jax.experimental import pallas as pl
from jax.experimental.pallas import tpu as pltpu
from jax.sharding import PartitionSpec as P

INV_TEMP = 1.25
MESH = pl.DeviceIdType.MESH
LANE = 128
TILE = 256
SEQS = 8
SLOTS = 3
ORDER = (6, 2, 4, 7, 3, 5, 1)
H_PART = 8
CHAINS = 4
WIDE = 25
MIB = 1024 * 1024
VMEM_A = 29
VMEM_B = 29


def peer_of(me, k):
    d = me
    for bit in (1, 2, 4):
        if k & bit:
            d = d + bit * (1 - 2 * ((me // bit) % 2))
    return d


def lanes(g):
    return pl.ds(pl.multiple_of(g * LANE, LANE), LANE)


def chunk(i):
    return pl.ds(pl.multiple_of(i * (WIDE * LANE), LANE), WIDE * LANE)


def chained(op, n, unroll, term, parts):
    def body(c, parts):
        return (*parts[1:], op(parts[0], term(c)))

    return lax.fori_loop(0, n, body, parts, unroll=unroll)


def across(op, reduce, parts):
    v = parts[0]
    for p in parts[1:]:
        v = op(v, p)
    return reduce(v, axis=1, keepdims=True)


def softmax_rows(tile, edge, put, n_src, full, tail, seqs):
    shard = full * LANE + tail
    shape = (seqs, LANE)
    lane = lax.broadcasted_iota(jnp.int32, shape, 1)
    parts = (tile(0, 0),) * CHAINS
    for s in range(n_src):
        parts = chained(jnp.maximum, full, full, lambda c: tile(s, c), parts)
        parts = (*parts[1:], jnp.maximum(parts[0], jnp.where(lane < tail, edge(s), -jnp.inf)))
    peak = jnp.broadcast_to(across(jnp.maximum, jnp.max, parts), shape)
    pend = tile(0, 0) * 0.0
    parts = (pend,) * CHAINS
    for s in range(n_src):
        off = s * shard % LANE
        base = s * shard // LANE

        def place(i, e, pend):
            r = pltpu.roll(e, off, 1) if off else e
            v = jnp.where(lane < off, pend, r) if off else r
            return r, v

        def body(c, carry):
            pend, *parts = carry
            e = jnp.exp(tile(s, c) - peak)
            r, v = place(base + c, e, pend)
            put(base + c, v)
            return (r, *parts[1:], parts[0] + e)

        pend, *parts = lax.fori_loop(0, full, body, (pend, *parts), unroll=full)
        e = jnp.where(lane < tail, jnp.exp(edge(s) - peak), 0.0)
        parts = [*parts[1:], parts[0] + e]
        _, pend = place(base + full, e, pend)
        if off + tail == LANE:
            put(base + full, pend)
    return 1.0 / across(jnp.add, jnp.sum, parts)


def fold(op, parts, wide):
    for k in range(0, wide.shape[1], LANE):
        parts = (*parts[1:], op(parts[0], wide[:, k:k + LANE]))
    return parts


def finish_bonus(get, put, inv, n_g):
    def body(i, carry):
        put(i, get(i) * inv)
        return carry

    lax.fori_loop(0, n_g // WIDE, body, 0)


def token_tile(token, seqs):
    shape = (seqs, LANE)
    row = lax.broadcasted_iota(jnp.int32, shape, 0)
    x = jnp.zeros(shape, jnp.int32)
    for b in range(seqs):
        x = jnp.where(row == b, token(b), x)
    return x - lax.broadcasted_iota(jnp.int32, shape, 1)


def excess_rows_with_picks(get, q_tile, x, inv, n_g):
    def body(i, carry):
        p_pick, q_pick, *parts = carry
        p, q = get(i) * inv, q_tile(i)
        for k in range(WIDE):
            hit = x == (i * WIDE + k) * LANE
            p_pick = jnp.where(hit, p[:, k * LANE:(k + 1) * LANE], p_pick)
            q_pick = jnp.where(hit, q[:, k * LANE:(k + 1) * LANE], q_pick)
        return (p_pick, q_pick, *fold(jnp.add, tuple(parts), jnp.maximum(p - q, 0.0)))

    zero = get(0)[:, :LANE] * 0.0
    p_pick, q_pick, *parts = lax.fori_loop(0, n_g // WIDE, body, (zero,) * (CHAINS + 2))
    return 1.0 / across(jnp.add, jnp.sum, parts), accept_column(p_pick, q_pick)


def accept_column(p_pick, q_pick):
    return jnp.minimum(1.0, jnp.sum(p_pick, axis=1, keepdims=True) / jnp.sum(q_pick, axis=1, keepdims=True))


def residual_rows(get, put, q_tile, inv, scale, n_g):
    def body(i, carry):
        put(i, jnp.maximum(get(i) * inv - q_tile(i), 0.0) * scale)
        return carry

    lax.fori_loop(0, n_g // WIDE, body, 0)


def to_lanes(col, first, n_out):
    seqs = col.shape[0]
    wide = lax.broadcasted_iota(jnp.int32, (seqs, n_out), 1)
    deep = lax.broadcasted_iota(jnp.int32, (seqs, n_out), 0)
    return jnp.sum(jnp.where(wide == deep + first, jnp.broadcast_to(col, (seqs, n_out)), 0.0), axis=0, keepdims=True)


def prefixes(accepts):
    run, expected = accepts[0], accepts[0]
    for a in accepts[1:]:
        run = run * a
        expected = expected + run
    return expected


def exchange_kernel(x_in, h_ref, w_ref, q_ref, recv_ref, edge_ref, done_ref, acc_ref, q_buf, token_ref, x_ref, stage, h_buf, w_buf, z_buf, send_buf, edge_buf,
                    x_sem, h_sem, w_sem, q_sem, send_sem, recv_sem, edge_send, edge_recv):
    me = lax.axis_index("tp")
    vocab, depth = w_ref.shape
    groups, n_dev = recv_ref.shape[:2]
    seqs, pos = stage.shape[2:4]
    draft = pos - 1
    seg = seqs * pos
    per_dev = groups * seqs
    n_tiles = pl.cdiv(vocab, TILE)
    last = vocab - (n_tiles - 1) * TILE
    lt = TILE // LANE
    full = vocab // LANE
    tail = vocab - full * LANE
    n_steps = groups * n_tiles
    lane = lax.broadcasted_iota(jnp.int32, (seqs, LANE), 1)

    def w_copy(u, size):
        slot = lax.rem(u, SLOTS)
        t = lax.rem(u, n_tiles)
        return pltpu.make_async_copy(w_ref.at[pl.ds(pl.multiple_of(t * TILE, TILE), size)], w_buf.at[slot, pl.ds(0, size)], w_sem.at[slot])

    def on_tile(u, act):
        t = lax.rem(u, n_tiles)

        @pl.when(t < n_tiles - 1)
        def _():
            act(w_copy(u, TILE))

        @pl.when(t == n_tiles - 1)
        def _():
            act(w_copy(u, last))

    def h_copy(g, c):
        src = h_ref.at[:, pl.ds(pl.multiple_of(g * seqs, seqs), seqs), :, lanes(c)]
        return pltpu.make_async_copy(src, stage.at[c], h_sem.at[c // H_PART])

    def h_start(g):
        for c in range(depth // LANE):
            h_copy(g, c).start()

    def relayout(g):
        flat = stage.reshape(depth // LANE, n_dev * seg, LANE)

        def part(i, carry):
            part_ref = stage.at[pl.ds(i * H_PART, H_PART)]
            pltpu.make_async_copy(part_ref, part_ref, h_sem.at[i]).wait()

            def cols(c, carry):
                h_buf[:, lanes(i * H_PART + c)] = flat[i * H_PART + c]
                return carry

            return lax.fori_loop(0, H_PART, cols, carry, unroll=True)

        lax.fori_loop(0, depth // LANE // H_PART, part, 0)

    def q_copy(g, j):
        return pltpu.make_async_copy(q_ref.at[j, pl.ds(pl.multiple_of(g * seqs, seqs), seqs)], q_buf.at[j], q_sem.at[j])

    h_start(0)
    w_copy(0, TILE).start()
    w_copy(1, TILE).start()

    barrier = pltpu.get_barrier_semaphore()
    for k in range(1, n_dev):
        pl.semaphore_signal(barrier, inc=1, device_id={"tp": peer_of(me, k)}, device_id_type=MESH)

    pltpu.make_async_copy(x_in, x_ref, x_sem.at[0]).start()
    acc_ref[...] = jnp.zeros_like(acc_ref)
    relayout(0)
    h_start(1)
    pl.semaphore_wait(barrier, n_dev - 1)

    def send(g, t, width):
        for c in range(width):
            recv_ref[g, me, t * lt + c] = send_buf[t, c, pl.ds(pl.multiple_of(me * seg, seg), seg), :]
        for k in ORDER:
            d = peer_of(me, k)
            pltpu.make_async_remote_copy(
                src_ref=send_buf.at[t, pl.ds(0, width), pl.ds(pl.multiple_of(d * seg, seg), seg)],
                dst_ref=recv_ref.at[g, me, pl.ds(t * lt, width)],
                send_sem=send_sem.at[t],
                recv_sem=recv_sem.at[g, k - 1],
                device_id={"tp": d},
                device_id_type=MESH,
            ).start()

    def wait_sent(t, width):
        ref = send_buf.at[t, pl.ds(0, width), pl.ds(0, (n_dev - 1) * seg)]
        pltpu.make_async_remote_copy(
            src_ref=ref, dst_ref=ref, send_sem=send_sem.at[t], recv_sem=recv_sem.at[0, 0],
            device_id={"tp": peer_of(me, 1)}, device_id_type=MESH,
        ).wait_send()

    def send_edge(g):
        for d in range(n_dev):
            packed = z_buf[1, pl.ds(d * seg, seqs, stride=pos), :]
            for j in range(1, pos):
                v = pltpu.roll(z_buf[1, pl.ds(d * seg + j, seqs, stride=pos), :], j * tail, 1)
                packed = jnp.where(lane < j * tail, packed, v)
            edge_buf[g, d] = packed
        edge_ref[g, me] = edge_buf[g, me]
        for k in ORDER:
            d = peer_of(me, k)
            pltpu.make_async_remote_copy(
                src_ref=edge_buf.at[g, d],
                dst_ref=edge_ref.at[g, me],
                send_sem=edge_send.at[k - 1],
                recv_sem=edge_recv.at[g, k - 1],
                device_id={"tp": d},
                device_id_type=MESH,
            ).start()

    rest = full - (n_tiles - 1) * lt

    def step(u, carry):
        g = u // n_tiles
        t = lax.rem(u, n_tiles)
        slot = lax.rem(u, SLOTS)

        @pl.when((t == 0) & (g > 0))
        def _():
            relayout(g)

            @pl.when(g + 1 < groups)
            def _():
                h_start(g + 1)

        on_tile(u, lambda c: c.wait())

        @pl.when(u + 2 < n_steps)
        def _():
            on_tile(u + 2, lambda c: c.start())

        z = lax.dot_general(h_buf[...], w_buf[slot], (((1,), (1,)), ((), ())), preferred_element_type=jnp.float32) * INV_TEMP
        for c in range(lt):
            z_buf[c] = z[:, c * LANE:(c + 1) * LANE]

        @pl.when((g > 0) & (t < n_tiles - 1))
        def _():
            wait_sent(t, lt)

        @pl.when((g > 0) & (t == n_tiles - 1))
        def _():
            wait_sent(t, rest)

        for c in range(lt):
            for d in range(n_dev):
                for j in range(pos):
                    send_buf[t, c, pl.ds(d * seg + j * seqs, seqs), :] = z_buf[c, pl.ds(d * seg + j, seqs, stride=pos), :]

        @pl.when(t < n_tiles - 1)
        def _():
            send(g, t, lt)

        @pl.when(t == n_tiles - 1)
        def _():
            send(g, t, rest)
            send_edge(g)

        return carry

    lax.fori_loop(0, n_steps, step, 0)

    def wait_group(g):
        for k in ORDER:
            d = peer_of(me, k)
            for ref, ss, rs in ((recv_ref, edge_send, recv_sem), (edge_ref, edge_send, edge_recv)):
                pltpu.make_async_remote_copy(
                    src_ref=ref.at[g, d], dst_ref=ref.at[g, d], send_sem=ss.at[k - 1], recv_sem=rs.at[g, k - 1],
                    device_id={"tp": d}, device_id_type=MESH,
                ).wait_recv()

    pltpu.make_async_copy(x_in, x_ref, x_sem.at[0]).wait()
    for j in range(draft):
        q_copy(0, j).start()

    def finish(g, carry):
        wait_group(g)
        accepts = []
        for j in range(pos):
            def tile(s, c):
                return recv_ref[g, s, c, pl.ds(j * seqs, seqs), :]

            def edge(s):
                v = edge_ref[g, s]
                return pltpu.roll(v, LANE - j * tail, 1) if j else v

            def put(i, v):
                done_ref[g, j, :, lanes(i)] = v

            def get(i):
                return done_ref[g, j, :, chunk(i)]

            def put_wide(i, v):
                done_ref[g, j, :, chunk(i)] = v

            n_g = done_ref.shape[3] // LANE
            inv = softmax_rows(tile, edge, put, n_dev, full, tail, seqs)
            if j == draft:
                finish_bonus(get, put_wide, inv, n_g)
                continue
            q_copy(g, j).wait()
            def q_tile(i):
                return q_buf[j, :, chunk(i)]

            x = token_tile(lambda b: x_ref[j, me * per_dev + g * seqs + b], seqs)
            scale, accept = excess_rows_with_picks(get, q_tile, x, inv, n_g)
            accepts.append(accept)
            residual_rows(get, put_wide, q_tile, inv, scale, n_g)

            q_copy(g + 1, j).start()

        for j in range(draft):
            acc_ref[j:j + 1, :] += to_lanes(accepts[j], g * seqs, per_dev)
        acc_ref[draft:pos, :] += to_lanes(prefixes(accepts), g * seqs, per_dev)
        return carry

    lax.fori_loop(0, groups - 1, finish, 0)
    for j in range(draft):
        q_copy(groups - 1, j).wait()
        token_ref[j] = token_tile(lambda b: x_ref[j, me * per_dev + (groups - 1) * seqs + b], seqs)
    wait_group(groups - 1)

    for t in range(n_tiles):
        wait_sent(t, lt if t < n_tiles - 1 else rest)
    for k in ORDER:
        d = peer_of(me, k)
        ref = edge_ref.at[:, d]
        pltpu.make_async_remote_copy(
            src_ref=ref, dst_ref=ref, send_sem=edge_send.at[k - 1], recv_sem=edge_recv.at[0, k - 1],
            device_id={"tp": d}, device_id_type=MESH,
        ).wait_send()


def output_kernel(recv_ref, edge_ref, done_ref, part_ref, q_buf, token_ref, res_ref, bonus_ref, acc_ref, exp_ref, row_buf, acc_buf, exp_buf, out_sem,
                  small_sem):
    groups, n_dev, full = recv_ref.shape[:3]
    seqs = edge_ref.shape[2]
    pos = done_ref.shape[1]
    draft = pos - 1
    vocab = done_ref.shape[3]
    n_g = vocab // LANE
    tail = vocab // n_dev - full * LANE
    per_dev = groups * seqs
    g_last = groups - 1

    def out(g, j, src):
        dst = bonus_ref if j == draft else res_ref.at[j]
        return pltpu.make_async_copy(src, dst.at[pl.ds(g * seqs, seqs)], out_sem.at[g, j])

    for g in range(g_last):
        for j in range(pos):
            out(g, j, done_ref.at[g, j]).start()

    accepts = []
    for j in (draft, *range(draft)):
        def tile(s, c):
            return recv_ref[g_last, s, c, pl.ds(j * seqs, seqs), :]

        def edge(s):
            v = edge_ref[g_last, s]
            return pltpu.roll(v, LANE - j * tail, 1) if j else v

        def put(i, v):
            row_buf[j, :, lanes(i)] = v

        def get(i):
            return row_buf[j, :, chunk(i)]

        def put_wide(i, v):
            row_buf[j, :, chunk(i)] = v

        inv = softmax_rows(tile, edge, put, n_dev, full, tail, seqs)
        if j == draft:
            finish_bonus(get, put_wide, inv, n_g)
        else:
            def q_tile(i):
                return q_buf[j, :, chunk(i)]

            scale, accept = excess_rows_with_picks(get, q_tile, token_ref[j], inv, n_g)
            accepts.append(accept)
            residual_rows(get, put_wide, q_tile, inv, scale, n_g)
        out(g_last, j, row_buf.at[j]).start()

    for j in range(draft):
        acc_buf[j:j + 1, :] = part_ref[j:j + 1, :] + to_lanes(accepts[j], g_last * seqs, per_dev)
    exp_buf[...] = part_ref[draft:pos, :] + to_lanes(prefixes(accepts), g_last * seqs, per_dev)
    small = (pltpu.make_async_copy(acc_buf, acc_ref, small_sem.at[0]), pltpu.make_async_copy(exp_buf, exp_ref, small_sem.at[1]))
    for c in small:
        c.start()
    for g in range(groups):
        for j in range(pos):
            out(g, j, row_buf.at[j]).wait()
    for c in small:
        c.wait()


def solution(mesh):
    n = mesh.shape["tp"]

    def local_step(hidden, w_shard, q_rows, x_group):
        seq_dev, draft, vocab = q_rows.shape
        batch, pos, depth = hidden.shape
        shard = w_shard.shape[1]
        n_tiles = pl.cdiv(shard, TILE)
        groups = seq_dev // SEQS
        rows = n * SEQS * pos
        full = shard // LANE
        dma = pltpu.SemaphoreType.DMA
        in_hbm = pl.BlockSpec(memory_space=pltpu.HBM)
        in_vmem = pl.BlockSpec(memory_space=pltpu.VMEM)
        x_t = x_group.T
        q_hbm = pltpu.with_memory_space_constraint(q_rows.transpose(1, 0, 2), pltpu.HBM)

        handed_on = pl.pallas_call(
            exchange_kernel,
            out_shape=[
                pltpu.VMEM((groups, n, full, SEQS * pos, LANE), jnp.float32),
                pltpu.VMEM((groups, n, SEQS, LANE), jnp.float32),
                pltpu.VMEM((groups - 1, pos, SEQS, vocab), jnp.float32),
                pltpu.VMEM((pos, seq_dev), jnp.float32),
                pltpu.VMEM((draft, SEQS, vocab), jnp.float32),
                pltpu.VMEM((draft, SEQS, LANE), jnp.int32),
            ],
            in_specs=[in_hbm] * 4,
            out_specs=[in_vmem] * 6,
            scratch_shapes=[
                pltpu.SMEM((draft, batch), jnp.int32),
                pltpu.VMEM((depth // LANE, n, SEQS, pos, LANE), jnp.bfloat16),
                pltpu.VMEM((rows, depth), jnp.bfloat16),
                pltpu.VMEM((SLOTS, TILE, depth), jnp.bfloat16),
                pltpu.VMEM((TILE // LANE, rows, LANE), jnp.float32),
                pltpu.VMEM((n_tiles, TILE // LANE, rows, LANE), jnp.float32),
                pltpu.VMEM((groups, n, SEQS, LANE), jnp.float32),
                dma((1,)),
                dma((depth // LANE // H_PART,)),
                dma((SLOTS,)),
                dma((draft,)),
                dma((n_tiles,)),
                dma((groups, n - 1)),
                dma((n - 1,)),
                dma((groups, n - 1)),
            ],
            compiler_params=pltpu.CompilerParams(collective_id=0, has_side_effects=True, vmem_limit_bytes=VMEM_A * MIB),
            cost_estimate=pl.CostEstimate(flops=2 * batch * pos * depth * shard, bytes_accessed=2 * shard * depth, transcendentals=0),
            name="logits_exchange",
        )(x_t, hidden.reshape(n, seq_dev, pos, depth), w_shard.T, q_hbm)

        res, bonus, acc, expd = pl.pallas_call(
            output_kernel,
            out_shape=[
                jax.ShapeDtypeStruct((draft, seq_dev, vocab), jnp.float32),
                jax.ShapeDtypeStruct((seq_dev, vocab), jnp.float32),
                jax.ShapeDtypeStruct((draft, seq_dev), jnp.float32),
                jax.ShapeDtypeStruct((1, seq_dev), jnp.float32),
            ],
            in_specs=[in_vmem] * 6,
            out_specs=[in_hbm] * 4,
            scratch_shapes=[
                pltpu.VMEM((pos, SEQS, vocab), jnp.float32),
                pltpu.VMEM((draft, seq_dev), jnp.float32),
                pltpu.VMEM((1, seq_dev), jnp.float32),
                dma((groups, pos)),
                dma((2,)),
            ],
            compiler_params=pltpu.CompilerParams(vmem_limit_bytes=VMEM_B * MIB),
            name="write_outputs",
        )(*(pltpu.with_memory_space_constraint(a, pltpu.VMEM) for a in handed_on))
        return acc.T, expd.reshape(seq_dev), res.transpose(1, 0, 2), bonus

    return jax.shard_map(local_step, mesh=mesh,
                         in_specs=(P("dp", None, None), P(None, "tp"), P(("dp", "tp"), None, None), P("dp", None)),
                         out_specs=(P(("dp", "tp"), None), P(("dp", "tp")), P(("dp", "tp"), None, None), P(("dp", "tp"), None)),
                         check_vma=False)
```

```python
import jax
import jax.numpy as jnp
from jax import lax
from jax.experimental import pallas as pl
from jax.experimental.pallas import tpu as pltpu
from jax.sharding import PartitionSpec as P

INV_TEMP = 1.25
MESH = pl.DeviceIdType.MESH
LANE = 128
TILE = 256
SEQS = 8
SLOTS = 3
ORDER = (6, 2, 4, 7, 3, 5, 1)
H_PART = 8
CHAINS = 4
WIDE = 25
MIB = 1024 * 1024
VMEM_A = 29
VMEM_B = 29


def peer_of(me, k):
    d = me
    for bit in (1, 2, 4):
        if k & bit:
            d = d + bit * (1 - 2 * ((me // bit) % 2))
    return d


def lanes(g):
    return pl.ds(pl.multiple_of(g * LANE, LANE), LANE)


def chunk(i):
    return pl.ds(pl.multiple_of(i * (WIDE * LANE), LANE), WIDE * LANE)


def chained(op, n, unroll, term, parts):
    def body(c, parts):
        return (*parts[1:], op(parts[0], term(c)))

    return lax.fori_loop(0, n, body, parts, unroll=unroll)


def across(op, reduce, parts):
    v = parts[0]
    for p in parts[1:]:
        v = op(v, p)
    return reduce(v, axis=1, keepdims=True)


def softmax_rows(tile, edge, put, n_src, full, tail, seqs):
    shard = full * LANE + tail
    shape = (seqs, LANE)
    lane = lax.broadcasted_iota(jnp.int32, shape, 1)
    parts = (tile(0, 0),) * CHAINS
    for s in range(n_src):
        parts = chained(jnp.maximum, full, full, lambda c: tile(s, c), parts)
        parts = (*parts[1:], jnp.maximum(parts[0], jnp.where(lane < tail, edge(s), -jnp.inf)))
    peak = jnp.broadcast_to(across(jnp.maximum, jnp.max, parts), shape)
    pend = tile(0, 0) * 0.0
    parts = (pend,) * CHAINS
    for s in range(n_src):
        off = s * shard % LANE
        base = s * shard // LANE

        def place(i, e, pend):
            r = pltpu.roll(e, off, 1) if off else e
            v = jnp.where(lane < off, pend, r) if off else r
            return r, v

        def body(c, carry):
            pend, *parts = carry
            e = jnp.exp(tile(s, c) - peak)
            r, v = place(base + c, e, pend)
            put(base + c, v)
            return (r, *parts[1:], parts[0] + e)

        pend, *parts = lax.fori_loop(0, full, body, (pend, *parts), unroll=full)
        e = jnp.where(lane < tail, jnp.exp(edge(s) - peak), 0.0)
        parts = [*parts[1:], parts[0] + e]
        _, pend = place(base + full, e, pend)
        if off + tail == LANE:
            put(base + full, pend)
    return 1.0 / across(jnp.add, jnp.sum, parts)


def fold(op, parts, wide):
    for k in range(0, wide.shape[1], LANE):
        parts = (*parts[1:], op(parts[0], wide[:, k:k + LANE]))
    return parts


def finish_bonus(get, put, inv, n_g):
    def body(i, carry):
        put(i, get(i) * inv)
        return carry

    lax.fori_loop(0, n_g // WIDE, body, 0)


def token_tile(token, seqs):
    shape = (seqs, LANE)
    row = lax.broadcasted_iota(jnp.int32, shape, 0)
    x = jnp.zeros(shape, jnp.int32)
    for b in range(seqs):
        x = jnp.where(row == b, token(b), x)
    return x - lax.broadcasted_iota(jnp.int32, shape, 1)


def excess_rows_with_picks(get, q_tile, x, inv, n_g):
    def body(i, carry):
        p_pick, q_pick, *parts = carry
        p, q = get(i) * inv, q_tile(i)
        for k in range(WIDE):
            hit = x == (i * WIDE + k) * LANE
            p_pick = jnp.where(hit, p[:, k * LANE:(k + 1) * LANE], p_pick)
            q_pick = jnp.where(hit, q[:, k * LANE:(k + 1) * LANE], q_pick)
        return (p_pick, q_pick, *fold(jnp.add, tuple(parts), jnp.maximum(p - q, 0.0)))

    zero = get(0)[:, :LANE] * 0.0
    p_pick, q_pick, *parts = lax.fori_loop(0, n_g // WIDE, body, (zero,) * (CHAINS + 2))
    return 1.0 / across(jnp.add, jnp.sum, parts), accept_column(p_pick, q_pick)


def accept_column(p_pick, q_pick):
    return jnp.minimum(1.0, jnp.sum(p_pick, axis=1, keepdims=True) / jnp.sum(q_pick, axis=1, keepdims=True))


def residual_rows(get, put, q_tile, inv, scale, n_g):
    def body(i, carry):
        put(i, jnp.maximum(get(i) * inv - q_tile(i), 0.0) * scale)
        return carry

    lax.fori_loop(0, n_g // WIDE, body, 0)


def to_lanes(col, first, n_out):
    seqs = col.shape[0]
    wide = lax.broadcasted_iota(jnp.int32, (seqs, n_out), 1)
    deep = lax.broadcasted_iota(jnp.int32, (seqs, n_out), 0)
    return jnp.sum(jnp.where(wide == deep + first, jnp.broadcast_to(col, (seqs, n_out)), 0.0), axis=0, keepdims=True)


def prefixes(accepts):
    run, expected = accepts[0], accepts[0]
    for a in accepts[1:]:
        run = run * a
        expected = expected + run
    return expected


def exchange_kernel(x_in, h_ref, w_ref, q_ref, recv_ref, edge_ref, done_ref, acc_ref, q_buf, token_ref, x_ref, stage, h_buf, w_buf, z_buf, send_buf, edge_buf,
                    x_sem, h_sem, first_sem, w_sem, q_sem, send_sem, recv_sem, edge_send, edge_recv):
    me = lax.axis_index("tp")
    vocab, depth = w_ref.shape
    groups, n_dev = recv_ref.shape[:2]
    seqs, pos = stage.shape[2:4]
    draft = pos - 1
    seg = seqs * pos
    per_dev = groups * seqs
    n_tiles = pl.cdiv(vocab, TILE)
    last = vocab - (n_tiles - 1) * TILE
    lt = TILE // LANE
    full = vocab // LANE
    tail = vocab - full * LANE
    n_steps = groups * n_tiles
    lane = lax.broadcasted_iota(jnp.int32, (seqs, LANE), 1)

    def w_copy(u, size):
        slot = lax.rem(u, SLOTS)
        t = lax.rem(u, n_tiles)
        return pltpu.make_async_copy(w_ref.at[pl.ds(pl.multiple_of(t * TILE, TILE), size)], w_buf.at[slot, pl.ds(0, size)], w_sem.at[slot])

    def on_tile(u, act):
        t = lax.rem(u, n_tiles)

        @pl.when(t < n_tiles - 1)
        def _():
            act(w_copy(u, TILE))

        @pl.when(t == n_tiles - 1)
        def _():
            act(w_copy(u, last))

    def h_copy(g, c):
        src = h_ref.at[:, pl.ds(pl.multiple_of(g * seqs, seqs), seqs), :, lanes(c)]
        return pltpu.make_async_copy(src, stage.at[c], h_sem.at[c // H_PART])

    def h_start(g):
        for c in range(depth // LANE):
            h_copy(g, c).start()

    def relayout(g):
        flat = stage.reshape(depth // LANE, n_dev * seg, LANE)

        def part(i, carry):
            part_ref = stage.at[pl.ds(i * H_PART, H_PART)]
            pltpu.make_async_copy(part_ref, part_ref, h_sem.at[i]).wait()

            def cols(c, carry):
                h_buf[:, lanes(i * H_PART + c)] = flat[i * H_PART + c]
                return carry

            return lax.fori_loop(0, H_PART, cols, carry, unroll=True)

        lax.fori_loop(0, depth // LANE // H_PART, part, 0)

    def q_copy(g, j):
        return pltpu.make_async_copy(q_ref.at[j, pl.ds(pl.multiple_of(g * seqs, seqs), seqs)], q_buf.at[j], q_sem.at[j])

    def first_w(c):
        rows = pl.ds(pl.multiple_of(c * LANE, LANE), LANE)
        return pltpu.make_async_copy(w_ref.at[rows], w_buf.at[0, rows], first_sem.at[c])

    first_w(0).start()
    h_start(0)
    first_w(1).start()
    w_copy(1, TILE).start()

    barrier = pltpu.get_barrier_semaphore()
    for k in range(1, n_dev):
        pl.semaphore_signal(barrier, inc=1, device_id={"tp": peer_of(me, k)}, device_id_type=MESH)

    pltpu.make_async_copy(x_in, x_ref, x_sem.at[0]).start()
    acc_ref[...] = jnp.zeros_like(acc_ref)

    def send(g, t, first, width):
        for c in range(width):
            recv_ref[g, me, t * lt + first + c] = send_buf[t, first + c, pl.ds(pl.multiple_of(me * seg, seg), seg), :]
        for k in ORDER:
            d = peer_of(me, k)
            pltpu.make_async_remote_copy(
                src_ref=send_buf.at[t, pl.ds(first, width), pl.ds(pl.multiple_of(d * seg, seg), seg)],
                dst_ref=recv_ref.at[g, me, pl.ds(t * lt + first, width)],
                send_sem=send_sem.at[t],
                recv_sem=recv_sem.at[g, k - 1],
                device_id={"tp": d},
                device_id_type=MESH,
            ).start()

    def wait_sent(t, width):
        ref = send_buf.at[t, pl.ds(0, width), pl.ds(0, (n_dev - 1) * seg)]
        pltpu.make_async_remote_copy(
            src_ref=ref, dst_ref=ref, send_sem=send_sem.at[t], recv_sem=recv_sem.at[0, 0],
            device_id={"tp": peer_of(me, 1)}, device_id_type=MESH,
        ).wait_send()

    def send_edge(g):
        for d in range(n_dev):
            packed = z_buf[1, pl.ds(d * seg, seqs, stride=pos), :]
            for j in range(1, pos):
                v = pltpu.roll(z_buf[1, pl.ds(d * seg + j, seqs, stride=pos), :], j * tail, 1)
                packed = jnp.where(lane < j * tail, packed, v)
            edge_buf[g, d] = packed
        edge_ref[g, me] = edge_buf[g, me]
        for k in ORDER:
            d = peer_of(me, k)
            pltpu.make_async_remote_copy(
                src_ref=edge_buf.at[g, d],
                dst_ref=edge_ref.at[g, me],
                send_sem=edge_send.at[k - 1],
                recv_sem=edge_recv.at[g, k - 1],
                device_id={"tp": d},
                device_id_type=MESH,
            ).start()

    rest = full - (n_tiles - 1) * lt

    def product(h, w):
        return lax.dot_general(h, w, (((1,), (1,)), ((), ())), preferred_element_type=jnp.float32) * INV_TEMP

    def by_position(t, c):
        for d in range(n_dev):
            for j in range(pos):
                send_buf[t, c, pl.ds(d * seg + j * seqs, seqs), :] = z_buf[c, pl.ds(d * seg + j, seqs, stride=pos), :]

    relayout(0)

    def first_tile(c, carry):
        first_w(c).wait()
        z_buf[c] = product(h_buf[...], w_buf[0, pl.ds(pl.multiple_of(c * LANE, LANE), LANE)])
        by_position(0, c)

        @pl.when(c == 0)
        def _():
            h_start(1)
            w_copy(2, TILE).start()
            pl.semaphore_wait(barrier, n_dev - 1)

        send(0, 0, c, 1)
        return carry

    lax.fori_loop(0, lt, first_tile, 0)

    def step(u, carry):
        g = u // n_tiles
        t = lax.rem(u, n_tiles)
        slot = lax.rem(u, SLOTS)

        @pl.when((t == 0) & (g > 0))
        def _():
            relayout(g)

            @pl.when(g + 1 < groups)
            def _():
                h_start(g + 1)

        on_tile(u, lambda c: c.wait())

        @pl.when(u + 2 < n_steps)
        def _():
            on_tile(u + 2, lambda c: c.start())

        z = product(h_buf[...], w_buf[slot])
        for c in range(lt):
            z_buf[c] = z[:, c * LANE:(c + 1) * LANE]

        @pl.when((g > 0) & (t < n_tiles - 1))
        def _():
            wait_sent(t, lt)

        @pl.when((g > 0) & (t == n_tiles - 1))
        def _():
            wait_sent(t, rest)

        for c in range(lt):
            by_position(t, c)

        @pl.when(t < n_tiles - 1)
        def _():
            send(g, t, 0, lt)

        @pl.when(t == n_tiles - 1)
        def _():
            send(g, t, 0, rest)
            send_edge(g)

        return carry

    lax.fori_loop(1, n_steps, step, 0)

    def wait_group(g):
        for k in ORDER:
            d = peer_of(me, k)
            for ref, ss, rs in ((recv_ref, edge_send, recv_sem), (edge_ref, edge_send, edge_recv)):
                pltpu.make_async_remote_copy(
                    src_ref=ref.at[g, d], dst_ref=ref.at[g, d], send_sem=ss.at[k - 1], recv_sem=rs.at[g, k - 1],
                    device_id={"tp": d}, device_id_type=MESH,
                ).wait_recv()

    pltpu.make_async_copy(x_in, x_ref, x_sem.at[0]).wait()
    for j in range(draft):
        q_copy(0, j).start()

    def finish(g, carry):
        wait_group(g)
        accepts = []
        for j in range(pos):
            def tile(s, c):
                return recv_ref[g, s, c, pl.ds(j * seqs, seqs), :]

            def edge(s):
                v = edge_ref[g, s]
                return pltpu.roll(v, LANE - j * tail, 1) if j else v

            def put(i, v):
                done_ref[g, j, :, lanes(i)] = v

            def get(i):
                return done_ref[g, j, :, chunk(i)]

            def put_wide(i, v):
                done_ref[g, j, :, chunk(i)] = v

            n_g = done_ref.shape[3] // LANE
            inv = softmax_rows(tile, edge, put, n_dev, full, tail, seqs)
            if j == draft:
                finish_bonus(get, put_wide, inv, n_g)
                continue
            q_copy(g, j).wait()
            def q_tile(i):
                return q_buf[j, :, chunk(i)]

            x = token_tile(lambda b: x_ref[j, me * per_dev + g * seqs + b], seqs)
            scale, accept = excess_rows_with_picks(get, q_tile, x, inv, n_g)
            accepts.append(accept)
            residual_rows(get, put_wide, q_tile, inv, scale, n_g)

            q_copy(g + 1, j).start()

        for j in range(draft):
            acc_ref[j:j + 1, :] += to_lanes(accepts[j], g * seqs, per_dev)
        acc_ref[draft:pos, :] += to_lanes(prefixes(accepts), g * seqs, per_dev)
        return carry

    lax.fori_loop(0, groups - 1, finish, 0)
    for j in range(draft):
        q_copy(groups - 1, j).wait()
        token_ref[j] = token_tile(lambda b: x_ref[j, me * per_dev + (groups - 1) * seqs + b], seqs)
    wait_group(groups - 1)

    for t in range(n_tiles):
        wait_sent(t, lt if t < n_tiles - 1 else rest)
    for k in ORDER:
        d = peer_of(me, k)
        ref = edge_ref.at[:, d]
        pltpu.make_async_remote_copy(
            src_ref=ref, dst_ref=ref, send_sem=edge_send.at[k - 1], recv_sem=edge_recv.at[0, k - 1],
            device_id={"tp": d}, device_id_type=MESH,
        ).wait_send()


def output_kernel(recv_ref, edge_ref, done_ref, part_ref, q_buf, token_ref, res_ref, bonus_ref, acc_ref, exp_ref, row_buf, acc_buf, exp_buf, out_sem,
                  small_sem):
    groups, n_dev, full = recv_ref.shape[:3]
    seqs = edge_ref.shape[2]
    pos = done_ref.shape[1]
    draft = pos - 1
    vocab = done_ref.shape[3]
    n_g = vocab // LANE
    tail = vocab // n_dev - full * LANE
    per_dev = groups * seqs
    g_last = groups - 1

    def out(g, j, src):
        dst = bonus_ref if j == draft else res_ref.at[j]
        return pltpu.make_async_copy(src, dst.at[pl.ds(g * seqs, seqs)], out_sem.at[g, j])

    for g in range(g_last):
        for j in range(pos):
            out(g, j, done_ref.at[g, j]).start()

    accepts = []
    for j in (draft, *range(draft)):
        def tile(s, c):
            return recv_ref[g_last, s, c, pl.ds(j * seqs, seqs), :]

        def edge(s):
            v = edge_ref[g_last, s]
            return pltpu.roll(v, LANE - j * tail, 1) if j else v

        def put(i, v):
            row_buf[j, :, lanes(i)] = v

        def get(i):
            return row_buf[j, :, chunk(i)]

        def put_wide(i, v):
            row_buf[j, :, chunk(i)] = v

        inv = softmax_rows(tile, edge, put, n_dev, full, tail, seqs)
        if j == draft:
            finish_bonus(get, put_wide, inv, n_g)
        else:
            def q_tile(i):
                return q_buf[j, :, chunk(i)]

            scale, accept = excess_rows_with_picks(get, q_tile, token_ref[j], inv, n_g)
            accepts.append(accept)
            residual_rows(get, put_wide, q_tile, inv, scale, n_g)
        out(g_last, j, row_buf.at[j]).start()

    for j in range(draft):
        acc_buf[j:j + 1, :] = part_ref[j:j + 1, :] + to_lanes(accepts[j], g_last * seqs, per_dev)
    exp_buf[...] = part_ref[draft:pos, :] + to_lanes(prefixes(accepts), g_last * seqs, per_dev)
    small = (pltpu.make_async_copy(acc_buf, acc_ref, small_sem.at[0]), pltpu.make_async_copy(exp_buf, exp_ref, small_sem.at[1]))
    for c in small:
        c.start()
    for g in range(groups):
        for j in range(pos):
            out(g, j, row_buf.at[j]).wait()
    for c in small:
        c.wait()


def solution(mesh):
    n = mesh.shape["tp"]

    def local_step(hidden, w_shard, q_rows, x_group):
        seq_dev, draft, vocab = q_rows.shape
        batch, pos, depth = hidden.shape
        shard = w_shard.shape[1]
        n_tiles = pl.cdiv(shard, TILE)
        groups = seq_dev // SEQS
        rows = n * SEQS * pos
        full = shard // LANE
        dma = pltpu.SemaphoreType.DMA
        in_hbm = pl.BlockSpec(memory_space=pltpu.HBM)
        in_vmem = pl.BlockSpec(memory_space=pltpu.VMEM)
        x_t = x_group.T
        q_hbm = pltpu.with_memory_space_constraint(q_rows.transpose(1, 0, 2), pltpu.HBM)

        handed_on = pl.pallas_call(
            exchange_kernel,
            out_shape=[
                pltpu.VMEM((groups, n, full, SEQS * pos, LANE), jnp.float32),
                pltpu.VMEM((groups, n, SEQS, LANE), jnp.float32),
                pltpu.VMEM((groups - 1, pos, SEQS, vocab), jnp.float32),
                pltpu.VMEM((pos, seq_dev), jnp.float32),
                pltpu.VMEM((draft, SEQS, vocab), jnp.float32),
                pltpu.VMEM((draft, SEQS, LANE), jnp.int32),
            ],
            in_specs=[in_hbm] * 4,
            out_specs=[in_vmem] * 6,
            scratch_shapes=[
                pltpu.SMEM((draft, batch), jnp.int32),
                pltpu.VMEM((depth // LANE, n, SEQS, pos, LANE), jnp.bfloat16),
                pltpu.VMEM((rows, depth), jnp.bfloat16),
                pltpu.VMEM((SLOTS, TILE, depth), jnp.bfloat16),
                pltpu.VMEM((TILE // LANE, rows, LANE), jnp.float32),
                pltpu.VMEM((n_tiles, TILE // LANE, rows, LANE), jnp.float32),
                pltpu.VMEM((groups, n, SEQS, LANE), jnp.float32),
                dma((1,)),
                dma((depth // LANE // H_PART,)),
                dma((TILE // LANE,)),
                dma((SLOTS,)),
                dma((draft,)),
                dma((n_tiles,)),
                dma((groups, n - 1)),
                dma((n - 1,)),
                dma((groups, n - 1)),
            ],
            compiler_params=pltpu.CompilerParams(collective_id=0, has_side_effects=True, vmem_limit_bytes=VMEM_A * MIB),
            cost_estimate=pl.CostEstimate(flops=2 * batch * pos * depth * shard, bytes_accessed=2 * shard * depth, transcendentals=0),
            name="logits_exchange",
        )(x_t, hidden.reshape(n, seq_dev, pos, depth), w_shard.T, q_hbm)

        res, bonus, acc, expd = pl.pallas_call(
            output_kernel,
            out_shape=[
                jax.ShapeDtypeStruct((draft, seq_dev, vocab), jnp.float32),
                jax.ShapeDtypeStruct((seq_dev, vocab), jnp.float32),
                jax.ShapeDtypeStruct((draft, seq_dev), jnp.float32),
                jax.ShapeDtypeStruct((1, seq_dev), jnp.float32),
            ],
            in_specs=[in_vmem] * 6,
            out_specs=[in_hbm] * 4,
            scratch_shapes=[
                pltpu.VMEM((pos, SEQS, vocab), jnp.float32),
                pltpu.VMEM((draft, seq_dev), jnp.float32),
                pltpu.VMEM((1, seq_dev), jnp.float32),
                dma((groups, pos)),
                dma((2,)),
            ],
            compiler_params=pltpu.CompilerParams(vmem_limit_bytes=VMEM_B * MIB),
            name="write_outputs",
        )(*(pltpu.with_memory_space_constraint(a, pltpu.VMEM) for a in handed_on))
        return acc.T, expd.reshape(seq_dev), res.transpose(1, 0, 2), bonus

    return jax.shard_map(local_step, mesh=mesh,
                         in_specs=(P("dp", None, None), P(None, "tp"), P(("dp", "tp"), None, None), P("dp", None)),
                         out_specs=(P(("dp", "tp"), None), P(("dp", "tp")), P(("dp", "tp"), None, None), P(("dp", "tp"), None)),
                         check_vma=False)
```

```python
import jax
import jax.numpy as jnp
from jax import lax
from jax.experimental import pallas as pl
from jax.experimental.pallas import tpu as pltpu
from jax.sharding import PartitionSpec as P

INV_TEMP = 1.25
MESH = pl.DeviceIdType.MESH
LANE = 128
TILE = 256
SEQS = 8
SLOTS = 3
ORDER = (6, 2, 4, 7, 3, 5, 1)
H_PART = 8
CHAINS = 4
WIDE = 25
MIB = 1024 * 1024
VMEM_A = 29
VMEM_B = 29


def peer_of(me, k):
    d = me
    for bit in (1, 2, 4):
        if k & bit:
            d = d + bit * (1 - 2 * ((me // bit) % 2))
    return d


def lanes(g):
    return pl.ds(pl.multiple_of(g * LANE, LANE), LANE)


def chunk(i):
    return pl.ds(pl.multiple_of(i * (WIDE * LANE), LANE), WIDE * LANE)


def chained(op, n, unroll, term, parts):
    def body(c, parts):
        return (*parts[1:], op(parts[0], term(c)))

    return lax.fori_loop(0, n, body, parts, unroll=unroll)


def across(op, reduce, parts):
    v = parts[0]
    for p in parts[1:]:
        v = op(v, p)
    return reduce(v, axis=1, keepdims=True)


def softmax_rows(tile, edge, put, n_src, full, tail, seqs):
    shard = full * LANE + tail
    shape = (seqs, LANE)
    lane = lax.broadcasted_iota(jnp.int32, shape, 1)
    parts = (tile(0, 0),) * CHAINS
    for s in range(n_src):
        parts = chained(jnp.maximum, full, full, lambda c: tile(s, c), parts)
        parts = (*parts[1:], jnp.maximum(parts[0], jnp.where(lane < tail, edge(s), -jnp.inf)))
    peak = jnp.broadcast_to(across(jnp.maximum, jnp.max, parts), shape)
    pend = tile(0, 0) * 0.0
    parts = (pend,) * CHAINS
    for s in range(n_src):
        off = s * shard % LANE
        base = s * shard // LANE

        def place(i, e, pend):
            r = pltpu.roll(e, off, 1) if off else e
            v = jnp.where(lane < off, pend, r) if off else r
            return r, v

        def body(c, carry):
            pend, *parts = carry
            e = jnp.exp(tile(s, c) - peak)
            r, v = place(base + c, e, pend)
            put(base + c, v)
            return (r, *parts[1:], parts[0] + e)

        pend, *parts = lax.fori_loop(0, full, body, (pend, *parts), unroll=full)
        e = jnp.where(lane < tail, jnp.exp(edge(s) - peak), 0.0)
        parts = [*parts[1:], parts[0] + e]
        _, pend = place(base + full, e, pend)
        if off + tail == LANE:
            put(base + full, pend)
    return 1.0 / across(jnp.add, jnp.sum, parts)


def fold(op, parts, wide):
    for k in range(0, wide.shape[1], LANE):
        parts = (*parts[1:], op(parts[0], wide[:, k:k + LANE]))
    return parts


def finish_bonus(get, put, inv, n_g):
    def body(i, carry):
        put(i, get(i) * inv)
        return carry

    lax.fori_loop(0, n_g // WIDE, body, 0)


def token_tile(token, seqs):
    shape = (seqs, LANE)
    row = lax.broadcasted_iota(jnp.int32, shape, 0)
    x = jnp.zeros(shape, jnp.int32)
    for b in range(seqs):
        x = jnp.where(row == b, token(b), x)
    return x - lax.broadcasted_iota(jnp.int32, shape, 1)


def excess_rows_with_picks(get, q_tile, x, inv, n_g):
    def body(i, carry):
        p_pick, q_pick, *parts = carry
        p, q = get(i) * inv, q_tile(i)
        for k in range(WIDE):
            hit = x == (i * WIDE + k) * LANE
            p_pick = jnp.where(hit, p[:, k * LANE:(k + 1) * LANE], p_pick)
            q_pick = jnp.where(hit, q[:, k * LANE:(k + 1) * LANE], q_pick)
        return (p_pick, q_pick, *fold(jnp.add, tuple(parts), jnp.maximum(p - q, 0.0)))

    zero = get(0)[:, :LANE] * 0.0
    p_pick, q_pick, *parts = lax.fori_loop(0, n_g // WIDE, body, (zero,) * (CHAINS + 2))
    return 1.0 / across(jnp.add, jnp.sum, parts), accept_column(p_pick, q_pick)


def accept_column(p_pick, q_pick):
    return jnp.minimum(1.0, jnp.sum(p_pick, axis=1, keepdims=True) / jnp.sum(q_pick, axis=1, keepdims=True))


def residual_rows(get, put, q_tile, inv, scale, first, last):
    def body(i, carry):
        put(i, jnp.maximum(get(i) * inv - q_tile(i), 0.0) * scale)
        return carry

    lax.fori_loop(first, last, body, 0)


def to_lanes(col, first, n_out):
    seqs = col.shape[0]
    wide = lax.broadcasted_iota(jnp.int32, (seqs, n_out), 1)
    deep = lax.broadcasted_iota(jnp.int32, (seqs, n_out), 0)
    return jnp.sum(jnp.where(wide == deep + first, jnp.broadcast_to(col, (seqs, n_out)), 0.0), axis=0, keepdims=True)


def prefixes(accepts):
    run, expected = accepts[0], accepts[0]
    for a in accepts[1:]:
        run = run * a
        expected = expected + run
    return expected


def exchange_kernel(x_in, h_ref, w_ref, q_ref, recv_ref, edge_ref, done_ref, acc_ref, q_buf, token_ref, x_ref, stage, h_buf, w_buf, z_buf, send_buf, edge_buf,
                    x_sem, h_sem, first_sem, w_sem, q_sem, send_sem, recv_sem, edge_send, edge_recv):
    me = lax.axis_index("tp")
    vocab, depth = w_ref.shape
    groups, n_dev = recv_ref.shape[:2]
    seqs, pos = stage.shape[2:4]
    draft = pos - 1
    seg = seqs * pos
    per_dev = groups * seqs
    n_tiles = pl.cdiv(vocab, TILE)
    last = vocab - (n_tiles - 1) * TILE
    lt = TILE // LANE
    full = vocab // LANE
    tail = vocab - full * LANE
    n_steps = groups * n_tiles
    lane = lax.broadcasted_iota(jnp.int32, (seqs, LANE), 1)

    def w_copy(u, size):
        slot = lax.rem(u, SLOTS)
        t = lax.rem(u, n_tiles)
        return pltpu.make_async_copy(w_ref.at[pl.ds(pl.multiple_of(t * TILE, TILE), size)], w_buf.at[slot, pl.ds(0, size)], w_sem.at[slot])

    def on_tile(u, act):
        t = lax.rem(u, n_tiles)

        @pl.when(t < n_tiles - 1)
        def _():
            act(w_copy(u, TILE))

        @pl.when(t == n_tiles - 1)
        def _():
            act(w_copy(u, last))

    def h_copy(g, c):
        src = h_ref.at[:, pl.ds(pl.multiple_of(g * seqs, seqs), seqs), :, lanes(c)]
        return pltpu.make_async_copy(src, stage.at[c], h_sem.at[c // H_PART])

    def h_start(g):
        for c in range(depth // LANE):
            h_copy(g, c).start()

    def relayout(g):
        flat = stage.reshape(depth // LANE, n_dev * seg, LANE)

        def part(i, carry):
            part_ref = stage.at[pl.ds(i * H_PART, H_PART)]
            pltpu.make_async_copy(part_ref, part_ref, h_sem.at[i]).wait()

            def cols(c, carry):
                h_buf[:, lanes(i * H_PART + c)] = flat[i * H_PART + c]
                return carry

            return lax.fori_loop(0, H_PART, cols, carry, unroll=True)

        lax.fori_loop(0, depth // LANE // H_PART, part, 0)

    def q_copy(g, j):
        return pltpu.make_async_copy(q_ref.at[j, pl.ds(pl.multiple_of(g * seqs, seqs), seqs)], q_buf.at[j], q_sem.at[j])

    def first_w(c):
        rows = pl.ds(pl.multiple_of(c * LANE, LANE), LANE)
        return pltpu.make_async_copy(w_ref.at[rows], w_buf.at[0, rows], first_sem.at[c])

    first_w(0).start()
    h_start(0)
    first_w(1).start()
    w_copy(1, TILE).start()

    barrier = pltpu.get_barrier_semaphore()
    for k in range(1, n_dev):
        pl.semaphore_signal(barrier, inc=1, device_id={"tp": peer_of(me, k)}, device_id_type=MESH)

    pltpu.make_async_copy(x_in, x_ref, x_sem.at[0]).start()
    acc_ref[...] = jnp.zeros_like(acc_ref)

    def send(g, t, first, width):
        for c in range(width):
            recv_ref[g, me, t * lt + first + c] = send_buf[t, first + c, pl.ds(pl.multiple_of(me * seg, seg), seg), :]
        for k in ORDER:
            d = peer_of(me, k)
            pltpu.make_async_remote_copy(
                src_ref=send_buf.at[t, pl.ds(first, width), pl.ds(pl.multiple_of(d * seg, seg), seg)],
                dst_ref=recv_ref.at[g, me, pl.ds(t * lt + first, width)],
                send_sem=send_sem.at[t],
                recv_sem=recv_sem.at[g, k - 1],
                device_id={"tp": d},
                device_id_type=MESH,
            ).start()

    def wait_sent(t, width):
        ref = send_buf.at[t, pl.ds(0, width), pl.ds(0, (n_dev - 1) * seg)]
        pltpu.make_async_remote_copy(
            src_ref=ref, dst_ref=ref, send_sem=send_sem.at[t], recv_sem=recv_sem.at[0, 0],
            device_id={"tp": peer_of(me, 1)}, device_id_type=MESH,
        ).wait_send()

    def send_edge(g):
        for d in range(n_dev):
            packed = z_buf[1, pl.ds(d * seg, seqs, stride=pos), :]
            for j in range(1, pos):
                v = pltpu.roll(z_buf[1, pl.ds(d * seg + j, seqs, stride=pos), :], j * tail, 1)
                packed = jnp.where(lane < j * tail, packed, v)
            edge_buf[g, d] = packed
        edge_ref[g, me] = edge_buf[g, me]
        for k in ORDER:
            d = peer_of(me, k)
            pltpu.make_async_remote_copy(
                src_ref=edge_buf.at[g, d],
                dst_ref=edge_ref.at[g, me],
                send_sem=edge_send.at[k - 1],
                recv_sem=edge_recv.at[g, k - 1],
                device_id={"tp": d},
                device_id_type=MESH,
            ).start()

    rest = full - (n_tiles - 1) * lt

    def product(h, w):
        return lax.dot_general(h, w, (((1,), (1,)), ((), ())), preferred_element_type=jnp.float32) * INV_TEMP

    def by_position(t, c):
        for d in range(n_dev):
            for j in range(pos):
                send_buf[t, c, pl.ds(d * seg + j * seqs, seqs), :] = z_buf[c, pl.ds(d * seg + j, seqs, stride=pos), :]

    relayout(0)

    def first_tile(c, carry):
        first_w(c).wait()
        z_buf[c] = product(h_buf[...], w_buf[0, pl.ds(pl.multiple_of(c * LANE, LANE), LANE)])
        by_position(0, c)

        @pl.when(c == 0)
        def _():
            h_start(1)
            w_copy(2, TILE).start()
            pl.semaphore_wait(barrier, n_dev - 1)

        send(0, 0, c, 1)
        return carry

    lax.fori_loop(0, lt, first_tile, 0)

    def step(u, carry):
        g = u // n_tiles
        t = lax.rem(u, n_tiles)
        slot = lax.rem(u, SLOTS)

        @pl.when((t == 0) & (g > 0))
        def _():
            relayout(g)

            @pl.when(g + 1 < groups)
            def _():
                h_start(g + 1)

        on_tile(u, lambda c: c.wait())

        @pl.when(u + 2 < n_steps)
        def _():
            on_tile(u + 2, lambda c: c.start())

        z = product(h_buf[...], w_buf[slot])
        for c in range(lt):
            z_buf[c] = z[:, c * LANE:(c + 1) * LANE]

        @pl.when((g > 0) & (t < n_tiles - 1))
        def _():
            wait_sent(t, lt)

        @pl.when((g > 0) & (t == n_tiles - 1))
        def _():
            wait_sent(t, rest)

        for c in range(lt):
            by_position(t, c)

        @pl.when(t < n_tiles - 1)
        def _():
            send(g, t, 0, lt)

        @pl.when(t == n_tiles - 1)
        def _():
            send(g, t, 0, rest)
            send_edge(g)

        return carry

    lax.fori_loop(1, n_steps, step, 0)

    def wait_group(g):
        for k in ORDER:
            d = peer_of(me, k)
            for ref, ss, rs in ((recv_ref, edge_send, recv_sem), (edge_ref, edge_send, edge_recv)):
                pltpu.make_async_remote_copy(
                    src_ref=ref.at[g, d], dst_ref=ref.at[g, d], send_sem=ss.at[k - 1], recv_sem=rs.at[g, k - 1],
                    device_id={"tp": d}, device_id_type=MESH,
                ).wait_recv()

    pltpu.make_async_copy(x_in, x_ref, x_sem.at[0]).wait()
    for j in range(draft):
        q_copy(0, j).start()

    def finish(g, carry):
        wait_group(g)
        accepts = []
        for j in range(pos):
            def tile(s, c):
                return recv_ref[g, s, c, pl.ds(j * seqs, seqs), :]

            def edge(s):
                v = edge_ref[g, s]
                return pltpu.roll(v, LANE - j * tail, 1) if j else v

            def put(i, v):
                done_ref[g, j, :, lanes(i)] = v

            def get(i):
                return done_ref[g, j, :, chunk(i)]

            def put_wide(i, v):
                done_ref[g, j, :, chunk(i)] = v

            n_g = done_ref.shape[3] // LANE
            inv = softmax_rows(tile, edge, put, n_dev, full, tail, seqs)
            if j == draft:
                finish_bonus(get, put_wide, inv, n_g)
                continue
            q_copy(g, j).wait()
            def q_tile(i):
                return q_buf[j, :, chunk(i)]

            x = token_tile(lambda b: x_ref[j, me * per_dev + g * seqs + b], seqs)
            scale, accept = excess_rows_with_picks(get, q_tile, x, inv, n_g)
            accepts.append(accept)
            residual_rows(get, put_wide, q_tile, inv, scale, 0, n_g // WIDE)

            q_copy(g + 1, j).start()

        for j in range(draft):
            acc_ref[j:j + 1, :] += to_lanes(accepts[j], g * seqs, per_dev)
        acc_ref[draft:pos, :] += to_lanes(prefixes(accepts), g * seqs, per_dev)
        return carry

    lax.fori_loop(0, groups - 1, finish, 0)
    for j in range(draft):
        q_copy(groups - 1, j).wait()
        token_ref[j] = token_tile(lambda b: x_ref[j, me * per_dev + (groups - 1) * seqs + b], seqs)
    wait_group(groups - 1)

    for t in range(n_tiles):
        wait_sent(t, lt if t < n_tiles - 1 else rest)
    for k in ORDER:
        d = peer_of(me, k)
        ref = edge_ref.at[:, d]
        pltpu.make_async_remote_copy(
            src_ref=ref, dst_ref=ref, send_sem=edge_send.at[k - 1], recv_sem=edge_recv.at[0, k - 1],
            device_id={"tp": d}, device_id_type=MESH,
        ).wait_send()


def output_kernel(recv_ref, edge_ref, done_ref, part_ref, q_buf, token_ref, res_ref, bonus_ref, acc_ref, exp_ref, row_buf, acc_buf, exp_buf, out_sem,
                  small_sem):
    groups, n_dev, full = recv_ref.shape[:3]
    seqs = edge_ref.shape[2]
    pos = done_ref.shape[1]
    draft = pos - 1
    vocab = done_ref.shape[3]
    n_g = vocab // LANE
    tail = vocab // n_dev - full * LANE
    per_dev = groups * seqs
    g_last = groups - 1

    def out(g, j, src):
        dst = bonus_ref if j == draft else res_ref.at[j]
        return pltpu.make_async_copy(src, dst.at[pl.ds(g * seqs, seqs)], out_sem.at[g, j])

    for g in range(g_last):
        for j in range(pos):
            out(g, j, done_ref.at[g, j]).start()

    accepts = []
    for j in (draft, *range(draft)):
        def tile(s, c):
            return recv_ref[g_last, s, c, pl.ds(j * seqs, seqs), :]

        def edge(s):
            v = edge_ref[g_last, s]
            return pltpu.roll(v, LANE - j * tail, 1) if j else v

        def put(i, v):
            row_buf[j, :, lanes(i)] = v

        def get(i):
            return row_buf[j, :, chunk(i)]

        def put_wide(i, v):
            row_buf[j, :, chunk(i)] = v

        inv = softmax_rows(tile, edge, put, n_dev, full, tail, seqs)
        if j == draft:
            finish_bonus(get, put_wide, inv, n_g)
            out(g_last, j, row_buf.at[j]).start()
        else:
            def q_tile(i):
                return q_buf[j, :, chunk(i)]

            scale, accept = excess_rows_with_picks(get, q_tile, token_ref[j], inv, n_g)
            accepts.append(accept)
            half = n_g // WIDE // 2
            for first, last in ((0, half), (half, n_g // WIDE)):
                residual_rows(get, put_wide, q_tile, inv, scale, first, last)
                cols = pl.ds(first * WIDE * LANE, (last - first) * WIDE * LANE)
                dst = res_ref.at[j, pl.ds(g_last * seqs, seqs), cols]
                pltpu.make_async_copy(row_buf.at[j, :, cols], dst, out_sem.at[g_last, j]).start()

    for j in range(draft):
        acc_buf[j:j + 1, :] = part_ref[j:j + 1, :] + to_lanes(accepts[j], g_last * seqs, per_dev)
    exp_buf[...] = part_ref[draft:pos, :] + to_lanes(prefixes(accepts), g_last * seqs, per_dev)
    small = (pltpu.make_async_copy(acc_buf, acc_ref, small_sem.at[0]), pltpu.make_async_copy(exp_buf, exp_ref, small_sem.at[1]))
    for c in small:
        c.start()
    for g in range(groups):
        for j in range(pos):
            out(g, j, row_buf.at[j]).wait()
    for c in small:
        c.wait()


def solution(mesh):
    n = mesh.shape["tp"]

    def local_step(hidden, w_shard, q_rows, x_group):
        seq_dev, draft, vocab = q_rows.shape
        batch, pos, depth = hidden.shape
        shard = w_shard.shape[1]
        n_tiles = pl.cdiv(shard, TILE)
        groups = seq_dev // SEQS
        rows = n * SEQS * pos
        full = shard // LANE
        dma = pltpu.SemaphoreType.DMA
        in_hbm = pl.BlockSpec(memory_space=pltpu.HBM)
        in_vmem = pl.BlockSpec(memory_space=pltpu.VMEM)
        x_t = x_group.T
        q_hbm = pltpu.with_memory_space_constraint(q_rows.transpose(1, 0, 2), pltpu.HBM)

        handed_on = pl.pallas_call(
            exchange_kernel,
            out_shape=[
                pltpu.VMEM((groups, n, full, SEQS * pos, LANE), jnp.float32),
                pltpu.VMEM((groups, n, SEQS, LANE), jnp.float32),
                pltpu.VMEM((groups - 1, pos, SEQS, vocab), jnp.float32),
                pltpu.VMEM((pos, seq_dev), jnp.float32),
                pltpu.VMEM((draft, SEQS, vocab), jnp.float32),
                pltpu.VMEM((draft, SEQS, LANE), jnp.int32),
            ],
            in_specs=[in_hbm] * 4,
            out_specs=[in_vmem] * 6,
            scratch_shapes=[
                pltpu.SMEM((draft, batch), jnp.int32),
                pltpu.VMEM((depth // LANE, n, SEQS, pos, LANE), jnp.bfloat16),
                pltpu.VMEM((rows, depth), jnp.bfloat16),
                pltpu.VMEM((SLOTS, TILE, depth), jnp.bfloat16),
                pltpu.VMEM((TILE // LANE, rows, LANE), jnp.float32),
                pltpu.VMEM((n_tiles, TILE // LANE, rows, LANE), jnp.float32),
                pltpu.VMEM((groups, n, SEQS, LANE), jnp.float32),
                dma((1,)),
                dma((depth // LANE // H_PART,)),
                dma((TILE // LANE,)),
                dma((SLOTS,)),
                dma((draft,)),
                dma((n_tiles,)),
                dma((groups, n - 1)),
                dma((n - 1,)),
                dma((groups, n - 1)),
            ],
            compiler_params=pltpu.CompilerParams(collective_id=0, has_side_effects=True, vmem_limit_bytes=VMEM_A * MIB),
            cost_estimate=pl.CostEstimate(flops=2 * batch * pos * depth * shard, bytes_accessed=2 * shard * depth, transcendentals=0),
            name="logits_exchange",
        )(x_t, hidden.reshape(n, seq_dev, pos, depth), w_shard.T, q_hbm)

        res, bonus, acc, expd = pl.pallas_call(
            output_kernel,
            out_shape=[
                jax.ShapeDtypeStruct((draft, seq_dev, vocab), jnp.float32),
                jax.ShapeDtypeStruct((seq_dev, vocab), jnp.float32),
                jax.ShapeDtypeStruct((draft, seq_dev), jnp.float32),
                jax.ShapeDtypeStruct((1, seq_dev), jnp.float32),
            ],
            in_specs=[in_vmem] * 6,
            out_specs=[in_hbm] * 4,
            scratch_shapes=[
                pltpu.VMEM((pos, SEQS, vocab), jnp.float32),
                pltpu.VMEM((draft, seq_dev), jnp.float32),
                pltpu.VMEM((1, seq_dev), jnp.float32),
                dma((groups, pos)),
                dma((2,)),
            ],
            compiler_params=pltpu.CompilerParams(vmem_limit_bytes=VMEM_B * MIB),
            name="write_outputs",
        )(*(pltpu.with_memory_space_constraint(a, pltpu.VMEM) for a in handed_on))
        return acc.T, expd.reshape(seq_dev), res.transpose(1, 0, 2), bonus

    return jax.shard_map(local_step, mesh=mesh,
                         in_specs=(P("dp", None, None), P(None, "tp"), P(("dp", "tp"), None, None), P("dp", None)),
                         out_specs=(P(("dp", "tp"), None), P(("dp", "tp")), P(("dp", "tp"), None, None), P(("dp", "tp"), None)),
                         check_vma=False)
```
